8 devices in a mesh: dp: 2 (over y, z), sp: 4 (over x, core).
Axes of the slice: x: 2, y: 2, z: 1, core: 2. Of those that a mesh axis runs over, the one named last changes fastest.
Arguments:
- x: bfloat16 [8192, 1024], P(('dp', 'sp')), parts along dimension 0
- gain: bfloat16 [1024], replicated
- wq: bfloat16 [1024, 4096], P('sp')
- wk: bfloat16 [1024, 4096], P('sp')
- wv: bfloat16 [1024, 4096], P('sp')
- wo: bfloat16 [4096, 1024], P('sp')
Outputs:
- output: bfloat16 [8192, 1024], P(('dp', 'sp')), parts along dimension 0
There are 2 independent parts. The reference program is written for one: setup_inputs(seed, part) draws one part's arguments, and reference() takes and returns one part's arrays. A program takes and returns all parts, laid end to end along the dimension named above; an argument that names none is the same for every part.
All inputs are finite; a program needn't handle non-finite values.
Results may differ from the reference program's by a relative error of at most 0.012.
Values are sent between devices in bfloat16 or wider.
A program may use at most 2 GiB of HBM per device.

```python
import jax
import jax.numpy as jnp
from jax import lax

ROWS = 4096
D = 1024
HEADS = 32
KV_HEADS = 32
HEAD = 128
THETA = 10000


def setup_inputs(seed: int = 0, part: int = 0) -> dict:
    kx, kn, kq, kk, kv, ko = jax.random.split(jax.random.key(seed), 6)

    def weights(key, rows, columns):
        return jax.random.normal(key, (rows, columns), jnp.float32) * rows**-0.5

    drawn = {
        "x": jax.random.normal(jax.random.fold_in(kx, part), (ROWS, D), jnp.float32),
        "gain": 1 + 0.1 * jax.random.normal(kn, (D,), jnp.float32),
        "wq": 2 * weights(kq, D, HEADS * HEAD),
        "wk": 2 * weights(kk, D, KV_HEADS * HEAD),
        "wv": 4 * weights(kv, D, KV_HEADS * HEAD),
        "wo": weights(ko, HEADS * HEAD, D),
    }
    return {k: v.astype(jnp.bfloat16) for k, v in drawn.items()}


def normed(x, gain):
    wide = x.astype(jnp.float32)
    scale = lax.rsqrt(jnp.mean(wide * wide, -1, keepdims=True) + 1e-6)
    return (wide * scale * gain.astype(jnp.float32)).astype(jnp.bfloat16)


def turned(t, place, theta):
    half = t.shape[-1] // 2
    angle = place.astype(jnp.float32)[:, None] * theta ** (-jnp.arange(half, dtype=jnp.float32) / half)
    cos, sin = jnp.cos(angle)[:, None], jnp.sin(angle)[:, None]
    a, b = t[..., :half].astype(jnp.float32), t[..., half:].astype(jnp.float32)
    return jnp.concatenate([a * cos - b * sin, b * cos + a * sin], -1).astype(jnp.bfloat16)


def matmul(a, w):
    return jnp.dot(a, w, preferred_element_type=jnp.float32).astype(jnp.bfloat16)


def einsum(form, a, b):
    return jnp.einsum(form, a.astype(jnp.float32), b.astype(jnp.float32))


def attention(q, k, v):
    scores = einsum("tgsd,ugd->gstu", q, k) * q.shape[-1] ** -0.5
    token = jnp.arange(q.shape[0])
    scores = jnp.where(token[:, None] >= token, scores, -jnp.inf)
    weights = jax.nn.softmax(scores, -1).astype(jnp.bfloat16)
    return einsum("gstu,ugd->tgsd", weights, v).astype(jnp.bfloat16)


def reference(x, gain, wq, wk, wv, wo):
    a, place = normed(x, gain), jnp.arange(ROWS)
    q = turned(matmul(a, wq).reshape(ROWS, HEADS, HEAD), place, THETA).reshape(ROWS, KV_HEADS, -1, HEAD)
    k = turned(matmul(a, wk).reshape(ROWS, KV_HEADS, HEAD), place, THETA)
    v = matmul(a, wv).reshape(ROWS, KV_HEADS, HEAD)
    seen = attention(q, k, v).reshape(ROWS, HEADS * HEAD)
    return (x.astype(jnp.float32) + jnp.dot(seen, wo, preferred_element_type=jnp.float32)).astype(jnp.bfloat16)
```

```python
import functools

import jax
import jax.numpy as jnp
import numpy as np
from jax import lax
from jax.experimental import pallas as pl
from jax.experimental.pallas import tpu as pltpu
from jax.sharding import PartitionSpec as P

HEAD = 128
THETA = 10000
NEG = -1e30
HIDDEN = 2 * NEG
LOG2E = 1.4426950408889634
B = 512
QUAD = 4
MESH = pl.DeviceIdType.MESH


def _dot(a, b, ca, cb):
    return lax.dot_general(a, b, (((ca,), (cb,)), ((), ())), preferred_element_type=jnp.float32)


def _angles():
    freq = np.float64(THETA) ** (-np.arange(64) / 64)
    freq = np.concatenate([freq, freq])
    sign = np.concatenate([-np.ones(64), np.ones(64)])
    coarse = 64 * np.arange(64)[:, None] * freq
    fine = np.arange(64)[:, None] * freq
    out = np.stack([np.cos(coarse), np.sin(coarse) * sign, np.cos(fine), np.sin(fine) * sign])
    return jnp.asarray(out.astype(np.float32))


def _kernel(x_hbm, gain_ref, ang_ref, wq_hbm, wk_hbm, wv_hbm, wo_hbm, out_hbm,
            xs, a_loc, w, wo, k_s, vt_s, q_s, o_s, cos_s, sin_s, top_s, mix_s, y_own, from_mate, from_far, half_in,
            w_send, w_recv, w_fwd, x_loc, x_mate_send, x_mate, x_send, x_dir, x_fwd_send, x_fwd,
            mate_send, mate_recv, half_send, half_recv, far_send, far_recv, misc):
    me = lax.axis_index("sp")
    y = lax.axis_index("dp")
    xx, cc = lax.div(me, 2), lax.rem(me, 2)
    mate = 2 * xx + 1 - cc
    far = 2 * (1 - xx) + cc
    far0 = 2 * (1 - xx)
    weights = (wk_hbm, wv_hbm, wq_hbm)
    rows = B // 2
    depth = 256

    barrier = pltpu.get_barrier_semaphore()
    for peer in (mate, far, 2 * (1 - xx) + 1 - cc):
        pl.semaphore_signal(barrier, inc=1, device_id={"dp": y, "sp": peer}, device_id_type=MESH)
    pl.semaphore_signal(barrier, inc=1, device_id={"dp": 1 - y, "sp": me}, device_id_type=MESH)
    pl.semaphore_wait(barrier, 4)

    def remote(src, dst, send, recv, sp, dp=y):
        return pltpu.make_async_remote_copy(src_ref=src, dst_ref=dst, send_sem=send, recv_sem=recv, device_id={"dp": dp, "sp": sp},
                                            device_id_type=MESH)

    def w_place(m, hp, sender):
        return w.at[m, hp, pl.ds(pl.multiple_of(sender * depth, depth), depth), :]

    def w_columns(m, hp, owner):
        return weights[m].at[:, pl.ds(pl.multiple_of(owner * 1024 + hp * 256, 256), 256)]

    def w_to(m, hp, owner, n):
        return remote(w_columns(m, hp, owner), w_place(m, hp, me), w_send.at[m, hp, n], w_recv.at[m, hp, me], owner)

    def w_from(m, hp, sender):
        return remote(w_place(m, hp, sender), w_place(m, hp, sender), misc.at[0], w_recv.at[m, hp, sender], sender)

    def w_on(m, hp, n):
        place = w_place(m, hp, far0 + n)
        return remote(place, place, w_fwd.at[m, lax.div(hp, 2), n], w_recv.at[m, hp, far0 + n], me, 1 - y)

    def w_own(m, hp):
        return pltpu.make_async_copy(w_columns(m, hp, me), w_place(m, hp, me), w_recv.at[m, hp, me])

    def x_own(i):
        return pltpu.make_async_copy(x_hbm.at[pl.ds(i * B, B), :], xs.at[2 * me + i], x_loc.at[i])

    def x_to_mate(i):
        return remote(x_hbm.at[pl.ds(i * B, B), :], xs.at[2 * me + i], x_mate_send.at[i], x_mate.at[i], mate)

    def x_from_mate(i):
        return remote(xs.at[2 * mate + i], xs.at[2 * mate + i], misc.at[0], x_mate.at[i], mate)

    def x_half(b, c):
        return xs.at[b, pl.ds(pl.multiple_of(c * rows, rows), rows), :]

    def x_to_far(i):
        return remote(x_half(4 * xx + i, cc), x_half(4 * xx + i, cc), x_send.at[i], x_dir.at[i], far)

    def x_from_far(i):
        place = x_half(4 * (1 - xx) + i, cc)
        return remote(place, place, misc.at[0], x_dir.at[i], far)

    def x_on(i):
        place = x_half(4 * (1 - xx) + i, cc)
        return remote(place, place, x_fwd_send.at[i], x_fwd.at[i], mate)

    def x_on_from(i):
        place = x_half(4 * (1 - xx) + i, 1 - cc)
        return remote(place, place, misc.at[0], x_fwd.at[i], mate)

    def y_to_mate(i):
        return remote(a_loc.at[i], from_mate.at[lax.rem(i, 2)], mate_send.at[lax.rem(i, 2)], mate_recv.at[lax.rem(i, 2)], mate)

    def y_from_mate(i):
        return remote(from_mate.at[i], from_mate.at[i], misc.at[0], mate_recv.at[i], mate)

    def half_to_mate(i):
        return remote(x_half(4 * (1 - xx) + i, 1 - cc), half_in.at[i], half_send.at[i], half_recv.at[i], mate)

    def half_from_mate(i):
        return remote(half_in.at[i], half_in.at[i], misc.at[0], half_recv.at[i], mate)

    def y_to_far(i):
        owner = 2 * (1 - xx) + lax.div(i, 2)
        return remote(x_half(4 * (1 - xx) + i, cc), from_far.at[lax.rem(i, 2), cc], far_send.at[i], far_recv.at[lax.rem(i, 2), cc], owner)

    def y_from_far(i, c):
        return remote(from_far.at[i, c], from_far.at[i, c], misc.at[0], far_recv.at[i, c], far0 + c)

    def loop(n, body):
        lax.fori_loop(0, n, lambda i, _: (body(i), None)[1], None)

    def hp_at(it):
        return 2 * lax.div(it, 2) + jnp.where(lax.rem(it, 2) == 0, y, 1 - y)

    for n in range(2):
        hp = hp_at(2 * n)
        for m in range(3):
            w_to(m, hp, far0 + cc, 1).start()
            w_to(m, hp, far0 + 1 - cc, 2).start()
    for i in range(2):
        x_own(i).start()
        x_to_mate(i).start()
    for it in range(4):
        hp = hp_at(it)
        for m in range(3):
            w_own(m, hp).start()
            w_to(m, hp, mate, 0).start()
    wo_copy = pltpu.make_async_copy(wo_hbm, wo, misc.at[1])
    wo_copy.start()
    for i in range(2):
        x_own(i).wait()
    for i in range(2):
        x_from_mate(i).wait_recv()
    loop(4, lambda i: x_to_far(i).start())

    def norm(src, dst):
        def part(r):
            here = pl.ds(pl.multiple_of(r * 64, 64), 64)
            wide = src[here, :].astype(jnp.float32)
            scale = lax.rsqrt(jnp.mean(wide * wide, -1, keepdims=True) + 1e-6)
            dst[here, :] = (wide * scale * gain_ref[...].astype(jnp.float32)).astype(jnp.bfloat16)

        loop(B // 64, part)

    def turn_table(b):
        for r in range(B // 64):
            here = pl.ds(r * 64, 64)
            at = pl.ds(b * (B // 64) + r, 1)
            ch, sh, cf, sf = ang_ref[0, at, :], ang_ref[1, at, :], ang_ref[2], ang_ref[3]
            cos_s[here, :] = ch * cf - sh * sf
            sin_s[here, :] = sh * cf + ch * sf

    def turned(t):
        t = t.astype(jnp.float32)
        return (t * cos_s[...] + pltpu.roll(t, 64, 1) * sin_s[...]).astype(jnp.bfloat16)

    def project(a, hp, b, slot):
        t = _dot(a[...], w[0, hp], 1, 0).astype(jnp.bfloat16)
        for i in range(2):
            k_s[b, 2 * hp + i] = turned(t[:, i * HEAD : (i + 1) * HEAD])
        t = _dot(a[...], w[1, hp], 1, 0).astype(jnp.bfloat16)
        for i in range(2):
            vt_s[b, 2 * hp + i, 0:HEAD, :] = t[:, i * HEAD : (i + 1) * HEAD].T
        t = _dot(a[...], w[2, hp], 1, 0).astype(jnp.bfloat16)
        for i in range(2):
            q_s[slot, 2 * hp + i] = turned(t[:, i * HEAD : (i + 1) * HEAD])

    e = HEAD**-0.5 * LOG2E

    def attend(qb, slot, quad):
        top_s[...] = jnp.full(top_s.shape, NEG, jnp.float32)
        mix_s[...] = jnp.zeros(mix_s.shape, jnp.float32)

        def block(j, pieces, mask):
            scores = []
            for n, at, wide, keys in pieces:
                h = quad * QUAD + n
                s = _dot(k_s[j, h, 0:keys, :], q_s[slot, h, at : at + wide, :], 1, 1)
                if mask:
                    ok = lax.broadcasted_iota(jnp.int32, s.shape, 1) + at >= lax.broadcasted_iota(jnp.int32, s.shape, 0)
                    s = jnp.where(ok, s, HIDDEN)
                scores.append(s)
            weights, keeps = [], []
            for (n, at, wide, keys), s in zip(pieces, scores):
                old = top_s[n : n + 1, at : at + wide]
                top = jnp.maximum(old, s.max(axis=0, keepdims=True))
                top_s[n : n + 1, at : at + wide] = top
                weights.append(jnp.exp2((s - top) * e).astype(jnp.bfloat16))
                keeps.append(jnp.exp2((old - top) * e))
            for (n, at, wide, keys), p, keep in zip(pieces, weights, keeps):
                h = quad * QUAD + n
                mix_s[n, :, at : at + wide] = mix_s[n, :, at : at + wide] * keep + _dot(vt_s[j, h, :, 0:keys], p, 1, 0)

        whole = [(n, 0, B, B) for n in range(QUAD)]
        cut = [(n, at, B // 2, at + B // 2) for n in range(QUAD) for at in (0, B // 2)]
        lax.fori_loop(0, qb, lambda j, _: (block(j, whole, False), None)[1], None)
        block(qb, cut, True)
        for n in range(QUAD):
            out = mix_s[n, 0:HEAD, :] * (1 / mix_s[n, HEAD : HEAD + 1, :])
            o_s[:, pl.ds(pl.multiple_of((quad * QUAD + n) * HEAD, HEAD), HEAD)] = out.T.astype(jnp.bfloat16)

    def combine(i):
        def part(r):
            here = pl.ds(pl.multiple_of(cc * rows + r * 64, 64), 64)
            at = pl.ds(pl.multiple_of(r * 64, 64), 64)
            b = 4 * (1 - xx) + i
            xs[b, here, :] = (xs[b, here, :].astype(jnp.float32) + half_in[i, at, :].astype(jnp.float32)).astype(jnp.bfloat16)

        loop(rows // 64, part)

    vt_s[:, :, HEAD:, :] = jnp.ones(vt_s.shape[:2] + (vt_s.shape[2] - HEAD, B), jnp.bfloat16)
    loop(4, lambda i: norm(xs.at[4 * xx + i], a_loc.at[i]))

    def pair(it):
        hp = hp_at(it)
        straight = lax.rem(it, 2) == 0
        for m in range(3):
            w_own(m, hp).wait()
            w_from(m, hp, mate).wait_recv()
            for n in range(2):
                w_from(m, hp, far0 + n).wait_recv()

                @pl.when(straight)
                def _():
                    w_on(m, hp, n).start()

        def tokens(i):
            turn_table(4 * xx + i)
            project(a_loc.at[i], hp, 4 * xx + i, i)

        loop(4, tokens)

    loop(4, pair)
    wo_copy.wait()

    first = 2 * (1 - xx)

    def forward_x(i):
        x_from_far(i).wait_recv()
        x_on(i).start()

    @pl.when(xx == 1)
    def _():
        forward_x(0)

    def step(s):
        i = s - first
        away = (i >= 0) & (i < 4)
        qb = jnp.where(xx == 1, s, jnp.where(s < 2, s, jnp.where(s < 6, s + 2, s - 4)))
        here = qb - 4 * xx
        slot = jnp.where(away, 4, here)

        @pl.when(away)
        def _():
            x_on(i).wait_send()
            x_on_from(i).wait_recv()
            norm(xs.at[qb], o_s)
            turn_table(qb)
            loop(4, lambda hp: project(o_s, hp, qb, 4))

        def quad(n):
            attend(qb, slot, n)

            @pl.when((n == 0) & (i >= 1) & (i < 5))
            def _():
                half_from_mate(i - 1).wait_recv()
                combine(i - 1)
                y_to_far(i - 1).start()

        loop(8 // QUAD, quad)

        @pl.when((i >= -1) & (i < 3))
        def _():
            forward_x(i + 1)

        own = jnp.logical_not(away) & (lax.div(here, 2) == cc)

        def columns(n):
            cols = pl.ds(pl.multiple_of(n * 256, 256), 256)
            r = _dot(o_s[...], wo[:, cols], 1, 0)

            @pl.when(own)
            def _():
                y_own[lax.rem(here, 2), :, cols] = r

            @pl.when(away)
            def _():
                xs[qb, :, cols] = r.astype(jnp.bfloat16)

            @pl.when(jnp.logical_not(own | away))
            def _():
                a_loc[here, :, cols] = r.astype(jnp.bfloat16)

        loop(4, columns)

        @pl.when(away)
        def _():
            half_to_mate(i).start()

        @pl.when(jnp.logical_not(own | away))
        def _():
            y_to_mate(here).start()

    loop(8, step)

    for i in range(2):
        y_from_mate(i).wait_recv()
        for c in range(2):
            y_from_far(i, c).wait_recv()
            base = c * rows

            def part(r):
                here = pl.ds(pl.multiple_of(base + r * 32, 32), 32)
                at = pl.ds(pl.multiple_of(r * 32, 32), 32)
                f = jnp.float32
                total = y_own[i, here, :] + from_mate[i, here, :].astype(f) + from_far[i, c, at, :].astype(f)
                a_loc[2 * cc + i, here, :] = (xs[2 * me + i, here, :].astype(f) + total).astype(jnp.bfloat16)

            loop(rows // 32, part)
        pltpu.make_async_copy(a_loc.at[2 * cc + i], out_hbm.at[pl.ds(i * B, B), :], x_loc.at[i]).start()

    for i in range(2):
        x_to_mate(i).wait_send()
        y_to_mate(2 * (1 - cc) + i).wait_send()
    for it in range(4):
        hp = hp_at(it)
        for m in range(3):
            w_to(m, hp, mate, 0).wait_send()
            if it % 2 == 0:
                w_to(m, hp, far0 + cc, 1).wait_send()
                w_to(m, hp, far0 + 1 - cc, 2).wait_send()
                for n in range(2):
                    w_on(m, hp, n).wait_send()

    def last(i):
        x_to_far(i).wait_send()
        half_to_mate(i).wait_send()
        y_to_far(i).wait_send()

    loop(4, last)
    for i in range(2):
        pltpu.make_async_copy(a_loc.at[2 * cc + i], out_hbm.at[pl.ds(i * B, B), :], x_loc.at[i]).wait()


def solution(mesh):
    bf, f = jnp.bfloat16, jnp.float32
    dma = pltpu.SemaphoreType.DMA

    def step(x, gain, wq, wk, wv, wo):
        hbm = pl.BlockSpec(memory_space=pl.ANY)
        vmem = pl.BlockSpec(memory_space=pltpu.VMEM)
        return pl.pallas_call(
            _kernel,
            out_shape=jax.ShapeDtypeStruct(x.shape, bf),
            in_specs=[hbm, vmem, vmem, hbm, hbm, hbm, hbm],
            out_specs=hbm,
            scratch_shapes=[
                pltpu.VMEM((8, B, 1024), bf),
                pltpu.VMEM((4, B, 1024), bf),
                pltpu.VMEM((3, 4, 1024, 256), bf),
                pltpu.VMEM((1024, 1024), bf),
                pltpu.VMEM((8, 8, B, HEAD), bf),
                pltpu.VMEM((8, 8, HEAD + 16, B), bf),
                pltpu.VMEM((5, 8, B, HEAD), bf),
                pltpu.VMEM((B, 1024), bf),
                pltpu.VMEM((B, HEAD), f),
                pltpu.VMEM((B, HEAD), f),
                pltpu.VMEM((QUAD, B), f),
                pltpu.VMEM((QUAD, HEAD + 16, B), f),
                pltpu.VMEM((2, B, 1024), f),
                pltpu.VMEM((2, B, 1024), bf),
                pltpu.VMEM((2, 2, B // 2, 1024), bf),
                pltpu.VMEM((4, B // 2, 1024), bf),
                dma((3, 4, 3)), dma((3, 4, 4)), dma((3, 2, 2)),
                dma((2,)), dma((2,)), dma((2,)), dma((4,)), dma((4,)), dma((4,)), dma((4,)),
                dma((2,)), dma((2,)), dma((4,)), dma((4,)), dma((4,)), dma((2, 2)), dma((2,)),
            ],
            compiler_params=pltpu.CompilerParams(collective_id=0, has_side_effects=True, vmem_limit_bytes=67043328),
            name="layer",
        )(x, gain.reshape(1, -1), _angles(), wq, wk, wv, wo)

    tokens, whole = P(("dp", "sp"), None), P("sp", None)
    return jax.shard_map(
        step,
        mesh=mesh,
        in_specs=(tokens, P(None), whole, whole, whole, whole),
        out_specs=tokens,
        check_vma=False,
    )
```

```python
import functools

import jax
import jax.numpy as jnp
import numpy as np
from jax import lax
from jax.experimental import pallas as pl
from jax.experimental.pallas import tpu as pltpu
from jax.sharding import PartitionSpec as P

HEAD = 128
THETA = 10000
NEG = -1e30
HIDDEN = 2 * NEG
LOG2E = 1.4426950408889634
B = 512
QUAD = 4
MESH = pl.DeviceIdType.MESH


def _dot(a, b, ca, cb):
    return lax.dot_general(a, b, (((ca,), (cb,)), ((), ())), preferred_element_type=jnp.float32)


def _angles():
    freq = np.float64(THETA) ** (-np.arange(64) / 64)
    freq = np.concatenate([freq, freq])
    sign = np.concatenate([-np.ones(64), np.ones(64)])
    coarse = 64 * np.arange(64)[:, None] * freq
    fine = np.arange(64)[:, None] * freq
    out = np.stack([np.cos(coarse), np.sin(coarse) * sign, np.cos(fine), np.sin(fine) * sign])
    return jnp.asarray(out.astype(np.float32))


def _kernel(x_hbm, gain_ref, ang_ref, wq_hbm, wk_hbm, wv_hbm, wo_hbm, out_hbm,
            xs, a_loc, w, wo, k_s, vt_s, q_s, a_far, cos_s, sin_s, top_s, mix_s, s_s, peak_s, y_own, from_mate, from_far, half_in,
            w_send, w_recv, w_fwd, x_loc, x_mate_send, x_mate, x_send, x_dir, x_fwd_send, x_fwd,
            mate_send, mate_recv, half_send, half_recv, far_send, far_recv, misc):
    me = lax.axis_index("sp")
    y = lax.axis_index("dp")
    xx, cc = lax.div(me, 2), lax.rem(me, 2)
    mate = 2 * xx + 1 - cc
    far = 2 * (1 - xx) + cc
    far0 = 2 * (1 - xx)
    weights = (wk_hbm, wv_hbm, wq_hbm)
    rows = B // 2
    depth = 256

    barrier = pltpu.get_barrier_semaphore()
    for peer in (mate, far, 2 * (1 - xx) + 1 - cc):
        pl.semaphore_signal(barrier, inc=1, device_id={"dp": y, "sp": peer}, device_id_type=MESH)
    pl.semaphore_signal(barrier, inc=1, device_id={"dp": 1 - y, "sp": me}, device_id_type=MESH)
    pl.semaphore_wait(barrier, 4)

    def remote(src, dst, send, recv, sp, dp=y):
        return pltpu.make_async_remote_copy(src_ref=src, dst_ref=dst, send_sem=send, recv_sem=recv, device_id={"dp": dp, "sp": sp},
                                            device_id_type=MESH)

    def w_place(m, hp, sender):
        return w.at[m, hp, pl.ds(pl.multiple_of(sender * depth, depth), depth), :]

    def w_columns(m, hp, owner):
        return weights[m].at[:, pl.ds(pl.multiple_of(owner * 1024 + hp * 256, 256), 256)]

    def w_to(m, hp, owner, n):
        return remote(w_columns(m, hp, owner), w_place(m, hp, me), w_send.at[m, hp, n], w_recv.at[m, hp, me], owner)

    def w_from(m, hp, sender):
        return remote(w_place(m, hp, sender), w_place(m, hp, sender), misc.at[0], w_recv.at[m, hp, sender], sender)

    def w_on(m, hp, n):
        place = w_place(m, hp, far0 + n)
        return remote(place, place, w_fwd.at[m, lax.div(hp, 2), n], w_recv.at[m, hp, far0 + n], me, 1 - y)

    def w_own(m, hp):
        return pltpu.make_async_copy(w_columns(m, hp, me), w_place(m, hp, me), w_recv.at[m, hp, me])

    def x_own(i):
        return pltpu.make_async_copy(x_hbm.at[pl.ds(i * B, B), :], xs.at[2 * me + i], x_loc.at[i])

    def x_to_mate(i):
        return remote(x_hbm.at[pl.ds(i * B, B), :], xs.at[2 * me + i], x_mate_send.at[i], x_mate.at[i], mate)

    def x_from_mate(i):
        return remote(xs.at[2 * mate + i], xs.at[2 * mate + i], misc.at[0], x_mate.at[i], mate)

    def x_half(b, c):
        return xs.at[b, pl.ds(pl.multiple_of(c * rows, rows), rows), :]

    def x_to_far(i):
        return remote(x_half(4 * xx + i, cc), x_half(4 * xx + i, cc), x_send.at[i], x_dir.at[i], far)

    def x_from_far(i):
        place = x_half(4 * (1 - xx) + i, cc)
        return remote(place, place, misc.at[0], x_dir.at[i], far)

    def x_on(i):
        place = x_half(4 * (1 - xx) + i, cc)
        return remote(place, place, x_fwd_send.at[i], x_fwd.at[i], mate)

    def x_on_from(i):
        place = x_half(4 * (1 - xx) + i, 1 - cc)
        return remote(place, place, misc.at[0], x_fwd.at[i], mate)

    def y_to_mate(i):
        return remote(a_loc.at[i], from_mate.at[lax.rem(i, 2)], mate_send.at[lax.rem(i, 2)], mate_recv.at[lax.rem(i, 2)], mate)

    def y_from_mate(i):
        return remote(from_mate.at[i], from_mate.at[i], misc.at[0], mate_recv.at[i], mate)

    def half_to_mate(i):
        return remote(x_half(4 * (1 - xx) + i, 1 - cc), half_in.at[i], half_send.at[i], half_recv.at[i], mate)

    def half_from_mate(i):
        return remote(half_in.at[i], half_in.at[i], misc.at[0], half_recv.at[i], mate)

    def y_to_far(i):
        owner = 2 * (1 - xx) + lax.div(i, 2)
        return remote(x_half(4 * (1 - xx) + i, cc), from_far.at[lax.rem(i, 2), cc], far_send.at[i], far_recv.at[lax.rem(i, 2), cc], owner)

    def y_from_far(i, c):
        return remote(from_far.at[i, c], from_far.at[i, c], misc.at[0], far_recv.at[i, c], far0 + c)

    def loop(n, body):
        lax.fori_loop(0, n, lambda i, _: (body(i), None)[1], None)

    def hp_at(it):
        return 2 * lax.div(it, 2) + jnp.where(lax.rem(it, 2) == 0, y, 1 - y)

    for n in range(2):
        hp = hp_at(2 * n)
        for m in range(3):
            w_to(m, hp, far0 + cc, 1).start()
            w_to(m, hp, far0 + 1 - cc, 2).start()
    for i in range(2):
        x_own(i).start()
        x_to_mate(i).start()
    for it in range(4):
        hp = hp_at(it)
        for m in range(3):
            w_own(m, hp).start()
            w_to(m, hp, mate, 0).start()
    wo_copy = pltpu.make_async_copy(wo_hbm, wo, misc.at[1])
    wo_copy.start()
    for i in range(2):
        x_own(i).wait()
    for i in range(2):
        x_from_mate(i).wait_recv()
    loop(4, lambda i: x_to_far(i).start())

    gain = gain_ref[...].astype(jnp.float32)[None, :]

    def norm(src, dst):
        def part(r):
            here = pl.ds(pl.multiple_of(r * 64, 64), 64)
            wide = src[here, :].astype(jnp.float32)
            scale = lax.rsqrt(jnp.mean(wide * wide, -1, keepdims=True) + 1e-6)
            dst[here, :] = (wide * scale * gain).astype(jnp.bfloat16)

        loop(B // 64, part)

    def turn_table(b):
        for r in range(B // 64):
            here = pl.ds(r * 64, 64)
            at = pl.ds(b * (B // 64) + r, 1)
            ch, sh, cf, sf = ang_ref[0, at, :], ang_ref[1, at, :], ang_ref[2], ang_ref[3]
            cos_s[here, :] = ch * cf - sh * sf
            sin_s[here, :] = sh * cf + ch * sf

    def turned(t):
        t = t.astype(jnp.float32)
        return (t * cos_s[...] + pltpu.roll(t, 64, 1) * sin_s[...]).astype(jnp.bfloat16)

    def project(a, hp, b, slot):
        t = _dot(a[...], w[0, hp], 1, 0).astype(jnp.bfloat16)
        for i in range(2):
            k_s[b, 2 * hp + i] = turned(t[:, i * HEAD : (i + 1) * HEAD])
        t = _dot(a[...], w[1, hp], 1, 0).astype(jnp.bfloat16)
        for i in range(2):
            vt_s[b, 2 * hp + i, 0:HEAD, :] = t[:, i * HEAD : (i + 1) * HEAD].T
        t = _dot(a[...], w[2, hp], 1, 0).astype(jnp.bfloat16)
        for i in range(2):
            q_s[slot, 2 * hp + i] = turned(t[:, i * HEAD : (i + 1) * HEAD])

    e = HEAD**-0.5 * LOG2E

    def scores(j, slot, h, n):
        s = _dot(k_s[j, h], q_s[slot, h], 1, 1)
        peak_s[n : n + 1, :] = s.max(axis=0, keepdims=True)
        s_s[n] = s

    def attend(qb, slot, quad):
        top_s[...] = jnp.full(top_s.shape, NEG, jnp.float32)
        mix_s[...] = jnp.zeros(mix_s.shape, jnp.float32)

        @pl.when(quad == 0)
        def _():
            for n in range(QUAD):
                scores(0, slot, n, n)

        def whole(j):
            for n in range(QUAD):
                h = quad * QUAD + n
                old = top_s[n : n + 1, :]
                top = jnp.maximum(old, peak_s[n : n + 1, :])
                top_s[n : n + 1, :] = top
                p = jnp.exp2((s_s[n] - top) * e).astype(jnp.bfloat16)
                scores(j + 1, slot, h, n)
                mix_s[n] = mix_s[n] * jnp.exp2((old - top) * e) + _dot(vt_s[j, h], p, 1, 0)

        loop(qb, whole)
        after = 1 - quad
        half = B // 2
        for n in range(QUAD):
            h = quad * QUAD + n
            for at in (0, half):
                keys, cols = at + half, slice(at, at + half)
                s = s_s[n, 0:keys, cols]
                ok = lax.broadcasted_iota(jnp.int32, s.shape, 1) + at >= lax.broadcasted_iota(jnp.int32, s.shape, 0)
                s = jnp.where(ok, s, HIDDEN)
                old = top_s[n : n + 1, cols]
                top = jnp.maximum(old, s.max(axis=0, keepdims=True))
                p = jnp.exp2((s - top) * e).astype(jnp.bfloat16)
                mix_s[n, :, cols] = mix_s[n, :, cols] * jnp.exp2((old - top) * e) + _dot(vt_s[qb, h, :, 0:keys], p, 1, 0)
            scores(0, slot, after * QUAD + n, n)
        for n in range(QUAD):
            out = mix_s[n, 0:HEAD, :] * (1 / mix_s[n, HEAD : HEAD + 1, :])
            q_s[slot, quad * QUAD + n] = out.T.astype(jnp.bfloat16)

    def combine(i):
        def part(r):
            here = pl.ds(pl.multiple_of(cc * rows + r * 64, 64), 64)
            at = pl.ds(pl.multiple_of(r * 64, 64), 64)
            b = 4 * (1 - xx) + i
            xs[b, here, :] = (xs[b, here, :].astype(jnp.float32) + half_in[i, at, :].astype(jnp.float32)).astype(jnp.bfloat16)

        loop(rows // 64, part)

    vt_s[:, :, HEAD:, :] = jnp.ones(vt_s.shape[:2] + (vt_s.shape[2] - HEAD, B), jnp.bfloat16)
    loop(4, lambda i: norm(xs.at[4 * xx + i], a_loc.at[i]))

    def pair(it):
        hp = hp_at(it)
        straight = lax.rem(it, 2) == 0
        for m in range(3):
            w_own(m, hp).wait()
            w_from(m, hp, mate).wait_recv()
            for n in range(2):
                w_from(m, hp, far0 + n).wait_recv()

                @pl.when(straight)
                def _():
                    w_on(m, hp, n).start()

        def tokens(i):
            turn_table(4 * xx + i)
            project(a_loc.at[i], hp, 4 * xx + i, i)

        loop(4, tokens)

    loop(4, pair)
    wo_copy.wait()

    first = 2 * (1 - xx)

    def forward_x(i):
        x_from_far(i).wait_recv()
        x_on(i).start()

    @pl.when(xx == 1)
    def _():
        forward_x(0)

    def step(s):
        i = s - first
        away = (i >= 0) & (i < 4)
        qb = jnp.where(xx == 1, s, jnp.where(s < 2, s, jnp.where(s < 6, s + 2, s - 4)))
        here = qb - 4 * xx
        slot = jnp.where(away, 4, here)

        @pl.when(away)
        def _():
            x_on(i).wait_send()
            x_on_from(i).wait_recv()
            norm(xs.at[qb], a_far)
            turn_table(qb)
            loop(4, lambda hp: project(a_far, hp, qb, 4))

        def quad(n):
            attend(qb, slot, n)

            @pl.when((n == 0) & (i >= 1) & (i < 5))
            def _():
                half_from_mate(i - 1).wait_recv()
                combine(i - 1)
                y_to_far(i - 1).start()

        loop(8 // QUAD, quad)

        @pl.when((i >= -1) & (i < 3))
        def _():
            forward_x(i + 1)

        own = jnp.logical_not(away) & (lax.div(here, 2) == cc)

        def columns(n):
            cols = pl.ds(pl.multiple_of(n * 256, 256), 256)
            seen = jnp.concatenate([q_s[slot, h] for h in range(8)], axis=1)
            r = _dot(seen, wo[:, cols], 1, 0)

            @pl.when(own)
            def _():
                y_own[lax.rem(here, 2), :, cols] = r

            @pl.when(away)
            def _():
                xs[qb, :, cols] = r.astype(jnp.bfloat16)

            @pl.when(jnp.logical_not(own | away))
            def _():
                a_loc[here, :, cols] = r.astype(jnp.bfloat16)

        loop(4, columns)

        @pl.when(away)
        def _():
            half_to_mate(i).start()

        @pl.when(jnp.logical_not(own | away))
        def _():
            y_to_mate(here).start()

    loop(8, step)

    for i in range(2):
        y_from_mate(i).wait_recv()
        for c in range(2):
            y_from_far(i, c).wait_recv()
            base = c * rows

            def part(r):
                here = pl.ds(pl.multiple_of(base + r * 32, 32), 32)
                at = pl.ds(pl.multiple_of(r * 32, 32), 32)
                f = jnp.float32
                total = y_own[i, here, :] + from_mate[i, here, :].astype(f) + from_far[i, c, at, :].astype(f)
                a_loc[2 * cc + i, here, :] = (xs[2 * me + i, here, :].astype(f) + total).astype(jnp.bfloat16)

            loop(rows // 32, part)
        pltpu.make_async_copy(a_loc.at[2 * cc + i], out_hbm.at[pl.ds(i * B, B), :], x_loc.at[i]).start()

    for i in range(2):
        x_to_mate(i).wait_send()
        y_to_mate(2 * (1 - cc) + i).wait_send()
    for it in range(4):
        hp = hp_at(it)
        for m in range(3):
            w_to(m, hp, mate, 0).wait_send()
            if it % 2 == 0:
                w_to(m, hp, far0 + cc, 1).wait_send()
                w_to(m, hp, far0 + 1 - cc, 2).wait_send()
                for n in range(2):
                    w_on(m, hp, n).wait_send()

    def last(i):
        x_to_far(i).wait_send()
        half_to_mate(i).wait_send()
        y_to_far(i).wait_send()

    loop(4, last)
    for i in range(2):
        pltpu.make_async_copy(a_loc.at[2 * cc + i], out_hbm.at[pl.ds(i * B, B), :], x_loc.at[i]).wait()


def solution(mesh):
    bf, f = jnp.bfloat16, jnp.float32
    dma = pltpu.SemaphoreType.DMA

    def step(x, gain, wq, wk, wv, wo):
        hbm = pl.BlockSpec(memory_space=pl.ANY)
        vmem = pl.BlockSpec(memory_space=pltpu.VMEM)
        return pl.pallas_call(
            _kernel,
            out_shape=jax.ShapeDtypeStruct(x.shape, bf),
            in_specs=[hbm, vmem, vmem, hbm, hbm, hbm, hbm],
            out_specs=hbm,
            scratch_shapes=[
                pltpu.VMEM((8, B, 1024), bf),
                pltpu.VMEM((4, B, 1024), bf),
                pltpu.VMEM((3, 4, 1024, 256), bf),
                pltpu.VMEM((1024, 1024), bf),
                pltpu.VMEM((8, 8, B, HEAD), bf),
                pltpu.VMEM((8, 8, HEAD + 16, B), bf),
                pltpu.VMEM((5, 8, B, HEAD), bf),
                pltpu.VMEM((B, 1024), bf),
                pltpu.VMEM((B, HEAD), f),
                pltpu.VMEM((B, HEAD), f),
                pltpu.VMEM((QUAD, B), f),
                pltpu.VMEM((QUAD, HEAD + 16, B), f),
                pltpu.VMEM((QUAD, B, B), f),
                pltpu.VMEM((QUAD, B), f),
                pltpu.VMEM((2, B, 1024), f),
                pltpu.VMEM((2, B, 1024), bf),
                pltpu.VMEM((2, 2, B // 2, 1024), bf),
                pltpu.VMEM((4, B // 2, 1024), bf),
                dma((3, 4, 3)), dma((3, 4, 4)), dma((3, 2, 2)),
                dma((2,)), dma((2,)), dma((2,)), dma((4,)), dma((4,)), dma((4,)), dma((4,)),
                dma((2,)), dma((2,)), dma((4,)), dma((4,)), dma((4,)), dma((2, 2)), dma((2,)),
            ],
            compiler_params=pltpu.CompilerParams(collective_id=0, has_side_effects=True, vmem_limit_bytes=67043328),
            name="layer",
        )(x, gain, _angles(), wq, wk, wv, wo)

    tokens, whole = P(("dp", "sp"), None), P("sp", None)
    return jax.shard_map(
        step,
        mesh=mesh,
        in_specs=(tokens, P(None), whole, whole, whole, whole),
        out_specs=tokens,
        check_vma=False,
    )
```

```python
import functools

import jax
import jax.numpy as jnp
import numpy as np
from jax import lax
from jax.experimental import pallas as pl
from jax.experimental.pallas import tpu as pltpu
from jax.sharding import PartitionSpec as P

HEAD = 128
THETA = 10000
NEG = -1e30
HIDDEN = 2 * NEG
LOG2E = 1.4426950408889634
B = 512
QUAD = 4
MESH = pl.DeviceIdType.MESH


def _dot(a, b, ca, cb):
    return lax.dot_general(a, b, (((ca,), (cb,)), ((), ())), preferred_element_type=jnp.float32)


def _angles():
    freq = np.float64(THETA) ** (-np.arange(64) / 64)
    freq = np.concatenate([freq, freq])
    sign = np.concatenate([-np.ones(64), np.ones(64)])
    coarse = 64 * np.arange(64)[:, None] * freq
    fine = np.arange(64)[:, None] * freq
    out = np.stack([np.cos(coarse), np.sin(coarse) * sign, np.cos(fine), np.sin(fine) * sign])
    return jnp.asarray(out.astype(np.float32))


def _kernel(x_hbm, gain_ref, ang_ref, wq_hbm, wk_hbm, wv_hbm, wo_hbm, out_hbm,
            xs, a_loc, w, wo, k_s, vt_s, q_s, a_far, cos_s, sin_s, top_s, mix_s, s_s, peak_s, y_own, from_mate, from_far, half_in,
            w_send, w_recv, w_fwd, x_loc, x_mate_send, x_mate, x_send, x_dir, x_fwd_send, x_fwd,
            mate_send, mate_recv, half_send, half_recv, far_send, far_recv, misc):
    me = lax.axis_index("sp")
    y = lax.axis_index("dp")
    xx, cc = lax.div(me, 2), lax.rem(me, 2)
    mate = 2 * xx + 1 - cc
    far = 2 * (1 - xx) + cc
    far0 = 2 * (1 - xx)
    weights = (wk_hbm, wv_hbm, wq_hbm)
    rows = B // 2
    depth = 256

    barrier = pltpu.get_barrier_semaphore()
    for peer in (mate, far, 2 * (1 - xx) + 1 - cc):
        pl.semaphore_signal(barrier, inc=1, device_id={"dp": y, "sp": peer}, device_id_type=MESH)
    pl.semaphore_signal(barrier, inc=1, device_id={"dp": 1 - y, "sp": me}, device_id_type=MESH)
    pl.semaphore_wait(barrier, 4)

    def remote(src, dst, send, recv, sp, dp=y):
        return pltpu.make_async_remote_copy(src_ref=src, dst_ref=dst, send_sem=send, recv_sem=recv, device_id={"dp": dp, "sp": sp},
                                            device_id_type=MESH)

    def w_place(m, hp, sender):
        return w.at[m, hp, pl.ds(pl.multiple_of(sender * depth, depth), depth), :]

    def w_columns(m, hp, owner):
        return weights[m].at[:, pl.ds(pl.multiple_of(owner * 1024 + hp * 256, 256), 256)]

    def w_to(m, hp, owner, n):
        return remote(w_columns(m, hp, owner), w_place(m, hp, me), w_send.at[m, hp, n], w_recv.at[m, hp, me], owner)

    def w_from(m, hp, sender):
        return remote(w_place(m, hp, sender), w_place(m, hp, sender), misc.at[0], w_recv.at[m, hp, sender], sender)

    def w_on(m, hp, n):
        place = w_place(m, hp, far0 + n)
        return remote(place, place, w_fwd.at[m, lax.div(hp, 2), n], w_recv.at[m, hp, far0 + n], me, 1 - y)

    def w_own(m, hp):
        return pltpu.make_async_copy(w_columns(m, hp, me), w_place(m, hp, me), w_recv.at[m, hp, me])

    def x_own(i):
        return pltpu.make_async_copy(x_hbm.at[pl.ds(i * B, B), :], xs.at[2 * me + i], x_loc.at[i])

    def x_to_mate(i):
        return remote(x_hbm.at[pl.ds(i * B, B), :], xs.at[2 * me + i], x_mate_send.at[i], x_mate.at[i], mate)

    def x_from_mate(i):
        return remote(xs.at[2 * mate + i], xs.at[2 * mate + i], misc.at[0], x_mate.at[i], mate)

    def x_half(b, c):
        return xs.at[b, pl.ds(pl.multiple_of(c * rows, rows), rows), :]

    def x_to_far(i):
        return remote(x_half(4 * xx + i, cc), x_half(4 * xx + i, cc), x_send.at[i], x_dir.at[i], far)

    def x_from_far(i):
        place = x_half(4 * (1 - xx) + i, cc)
        return remote(place, place, misc.at[0], x_dir.at[i], far)

    def x_on(i):
        place = x_half(4 * (1 - xx) + i, cc)
        return remote(place, place, x_fwd_send.at[i], x_fwd.at[i], mate)

    def x_on_from(i):
        place = x_half(4 * (1 - xx) + i, 1 - cc)
        return remote(place, place, misc.at[0], x_fwd.at[i], mate)

    def y_to_mate(i):
        return remote(a_loc.at[i], from_mate.at[lax.rem(i, 2)], mate_send.at[lax.rem(i, 2)], mate_recv.at[lax.rem(i, 2)], mate)

    def y_from_mate(i):
        return remote(from_mate.at[i], from_mate.at[i], misc.at[0], mate_recv.at[i], mate)

    def half_to_mate(i):
        return remote(x_half(4 * (1 - xx) + i, 1 - cc), half_in.at[i], half_send.at[i], half_recv.at[i], mate)

    def half_from_mate(i):
        return remote(half_in.at[i], half_in.at[i], misc.at[0], half_recv.at[i], mate)

    def y_to_far(i):
        owner = 2 * (1 - xx) + lax.div(i, 2)
        return remote(x_half(4 * (1 - xx) + i, cc), from_far.at[lax.rem(i, 2), cc], far_send.at[i], far_recv.at[lax.rem(i, 2), cc], owner)

    def y_from_far(i, c):
        return remote(from_far.at[i, c], from_far.at[i, c], misc.at[0], far_recv.at[i, c], far0 + c)

    def loop(n, body):
        lax.fori_loop(0, n, lambda i, _: (body(i), None)[1], None)

    def hp_at(it):
        return 2 * lax.div(it, 2) + jnp.where(lax.rem(it, 2) == 0, y, 1 - y)

    def crossing(g):
        if isinstance(g, int) and g < 6:
            return [w_to(g % 3, hp_at(2 * (g // 3)), far0 + (cc if n == 1 else 1 - cc), n) for n in (1, 2)]
        return [x_to_far(g - 6)]

    def cross(g):
        for copy in crossing(g - 2):
            copy.wait_send()
        for copy in crossing(g):
            copy.start()

    for g in range(2):
        for copy in crossing(g):
            copy.start()
    for i in range(2):
        x_own(i).start()
        x_to_mate(i).start()
    for it in range(4):
        hp = hp_at(it)
        for m in range(3):
            w_own(m, hp).start()
            w_to(m, hp, mate, 0).start()
    wo_copy = pltpu.make_async_copy(wo_hbm, wo, misc.at[1])
    wo_copy.start()

    def arrive(m, hp, onward):
        for n in range(2):
            w_from(m, hp, far0 + n).wait_recv()
            if onward:
                w_on(m, hp, n).start()

    arrive(0, hp_at(0), True)
    cross(2)
    for i in range(2):
        x_own(i).wait()
    for i in range(2):
        x_from_mate(i).wait_recv()

    gain = gain_ref[...].astype(jnp.float32)[None, :]

    def norm(src, dst):
        def part(r):
            here = pl.ds(pl.multiple_of(r * 256, 256), 256)
            wide = src[here, :].astype(jnp.float32)
            scale = lax.rsqrt(jnp.mean(wide * wide, -1, keepdims=True) + 1e-6)
            dst[here, :] = (wide * scale * gain).astype(jnp.bfloat16)

        loop(B // 256, part)

    def turn_table(b):
        for r in range(B // 64):
            here = pl.ds(r * 64, 64)
            at = pl.ds(b * (B // 64) + r, 1)
            ch, sh, cf, sf = ang_ref[0, at, :], ang_ref[1, at, :], ang_ref[2], ang_ref[3]
            cos_s[here, :] = ch * cf - sh * sf
            sin_s[here, :] = sh * cf + ch * sf

    def turned(t):
        t = t.astype(jnp.float32)
        return (t * cos_s[...] + pltpu.roll(t, 64, 1) * sin_s[...]).astype(jnp.bfloat16)

    def project_one(a, m, hp, b, slot):
        t = _dot(a[...], w[m, hp], 1, 0).astype(jnp.bfloat16)
        for i in range(2):
            part = t[:, i * HEAD : (i + 1) * HEAD]
            if m == 0:
                k_s[b, 2 * hp + i] = turned(part)
            elif m == 1:
                vt_s[b, 2 * hp + i, 0:HEAD, :] = part.T
            else:
                q_s[slot, 2 * hp + i] = turned(part)

    def project(a, hp, b, slot):
        for m in range(3):
            project_one(a, m, hp, b, slot)

    e = HEAD**-0.5 * LOG2E

    def scores(j, slot, h, n):
        s = _dot(k_s[j, h], q_s[slot, h], 1, 1)
        peak_s[n : n + 1, :] = s.max(axis=0, keepdims=True)
        s_s[n] = s

    def attend(qb, slot, quad):
        top_s[...] = jnp.full(top_s.shape, NEG, jnp.float32)
        mix_s[...] = jnp.zeros(mix_s.shape, jnp.float32)

        @pl.when(quad == 0)
        def _():
            for n in range(QUAD):
                scores(0, slot, n, n)

        def whole(j):
            for n in range(QUAD):
                h = quad * QUAD + n
                old = top_s[n : n + 1, :]
                top = jnp.maximum(old, peak_s[n : n + 1, :])
                top_s[n : n + 1, :] = top
                p = jnp.exp2((s_s[n] - top) * e).astype(jnp.bfloat16)
                scores(j + 1, slot, h, n)
                mix_s[n] = mix_s[n] * jnp.exp2((old - top) * e) + _dot(vt_s[j, h], p, 1, 0)

        def two(t):
            whole(2 * t)
            whole(2 * t + 1)

        loop(lax.div(qb, 2), two)

        @pl.when(lax.rem(qb, 2) == 1)
        def _():
            whole(qb - 1)

        after = 1 - quad
        half = B // 2
        ok = lax.broadcasted_iota(jnp.int32, (half, half), 1) >= lax.broadcasted_iota(jnp.int32, (half, half), 0)
        for n in range(QUAD):
            h = quad * QUAD + n
            for at in (0, half):
                cols = slice(at, at + half)
                parts = [s_s[n, 0:half, cols], jnp.where(ok, s_s[n, half:B, cols], HIDDEN)] if at else [jnp.where(ok, s_s[n, 0:half, cols], HIDDEN)]
                old = top_s[n : n + 1, cols]
                top = old
                for part in parts:
                    top = jnp.maximum(top, part.max(axis=0, keepdims=True))
                p = jnp.concatenate([jnp.exp2((part - top) * e).astype(jnp.bfloat16) for part in parts], axis=0)
                mix_s[n, :, cols] = mix_s[n, :, cols] * jnp.exp2((old - top) * e) + _dot(vt_s[qb, h, :, 0 : at + half], p, 1, 0)
            scores(0, slot, after * QUAD + n, n)
        for n in range(QUAD):
            out = mix_s[n, 0:HEAD, :] * (1 / mix_s[n, HEAD : HEAD + 1, :])
            q_s[slot, quad * QUAD + n] = out.T.astype(jnp.bfloat16)

    def combine(i):
        def part(r):
            here = pl.ds(pl.multiple_of(cc * rows + r * 64, 64), 64)
            at = pl.ds(pl.multiple_of(r * 64, 64), 64)
            b = 4 * (1 - xx) + i
            xs[b, here, :] = (xs[b, here, :].astype(jnp.float32) + half_in[i, at, :].astype(jnp.float32)).astype(jnp.bfloat16)

        loop(rows // 64, part)

    vt_s[:, :, HEAD:, :] = jnp.ones(vt_s.shape[:2] + (vt_s.shape[2] - HEAD, B), jnp.bfloat16)
    loop(4, lambda i: norm(xs.at[4 * xx + i], a_loc.at[i]))

    def pair(it):
        hp = hp_at(it)
        for m in range(3):
            w_own(m, hp).wait()
            w_from(m, hp, mate).wait_recv()

        @pl.when(it == 0)
        def _():
            for m in (1, 2):
                arrive(m, hp, True)
                cross(2 + m)

        @pl.when(it == 1)
        def _():
            arrive(0, hp_at(2), True)
            cross(5)
            for m in range(3):
                arrive(m, hp, False)

        @pl.when(it == 2)
        def _():
            for m in (1, 2):
                arrive(m, hp, True)
                cross(5 + m)

        @pl.when(it == 3)
        def _():
            for m in range(3):
                arrive(m, hp, False)

        def tokens(t):
            for i in (2 * t, 2 * t + 1):
                turn_table(4 * xx + i)
                project(a_loc.at[i], hp, 4 * xx + i, i)

        loop(2, tokens)

    loop(4, pair)
    wo_copy.wait()

    first = 2 * (1 - xx)

    def forward_x(i):
        x_from_far(i).wait_recv()
        x_on(i).start()

    @pl.when(xx == 1)
    def _():
        forward_x(0)

    def step(s):
        @pl.when((s == 1) | (s == 2))
        def _():
            cross(s + 7)

        i = s - first
        away = (i >= 0) & (i < 4)
        qb = jnp.where(xx == 1, s, jnp.where(s < 2, s, jnp.where(s < 6, s + 2, s - 4)))
        here = qb - 4 * xx
        slot = jnp.where(away, 4, here)

        @pl.when(away)
        def _():
            x_on(i).wait_send()
            x_on_from(i).wait_recv()
            norm(xs.at[qb], a_far)
            turn_table(qb)
            for hp in range(4):
                project(a_far, hp, qb, 4)

        def quad(n):
            attend(qb, slot, n)

            @pl.when((n == 0) & (i >= 1) & (i < 5))
            def _():
                half_from_mate(i - 1).wait_recv()
                combine(i - 1)
                y_to_far(i - 1).start()

        loop(8 // QUAD, quad)

        @pl.when((i >= -1) & (i < 3))
        def _():
            forward_x(i + 1)

        own = jnp.logical_not(away) & (lax.div(here, 2) == cc)

        def output(store):
            seen = jnp.concatenate([q_s[slot, h] for h in range(8)], axis=1)
            for n in range(4):
                cols = slice(n * 256, n * 256 + 256)
                store(cols, _dot(seen, wo[:, cols], 1, 0))

        @pl.when(own)
        def _():
            def store(cols, r):
                y_own[lax.rem(here, 2), :, cols] = r

            output(store)

        @pl.when(away)
        def _():
            def store(cols, r):
                xs[qb, :, cols] = r.astype(jnp.bfloat16)

            output(store)

        @pl.when(jnp.logical_not(own | away))
        def _():
            def store(cols, r):
                a_loc[here, :, cols] = r.astype(jnp.bfloat16)

            output(store)

        @pl.when(away)
        def _():
            half_to_mate(i).start()

        @pl.when(jnp.logical_not(own | away))
        def _():
            y_to_mate(here).start()

    loop(8, step)

    for i in range(2):
        y_from_mate(i).wait_recv()
        for c in range(2):
            y_from_far(i, c).wait_recv()
            base = c * rows

            def part(r):
                here = pl.ds(pl.multiple_of(base + r * 32, 32), 32)
                at = pl.ds(pl.multiple_of(r * 32, 32), 32)
                f = jnp.float32
                total = y_own[i, here, :] + from_mate[i, here, :].astype(f) + from_far[i, c, at, :].astype(f)
                a_loc[2 * cc + i, here, :] = (xs[2 * me + i, here, :].astype(f) + total).astype(jnp.bfloat16)

            loop(rows // 32, part)
        pltpu.make_async_copy(a_loc.at[2 * cc + i], out_hbm.at[pl.ds(i * B, B), :], x_loc.at[i]).start()

    for i in range(2):
        x_to_mate(i).wait_send()
        y_to_mate(2 * (1 - cc) + i).wait_send()
    for it in range(4):
        hp = hp_at(it)
        for m in range(3):
            w_to(m, hp, mate, 0).wait_send()
            if it % 2 == 0:
                for n in range(2):
                    w_on(m, hp, n).wait_send()

    for i in (2, 3):
        x_to_far(i).wait_send()

    def last(i):
        half_to_mate(i).wait_send()
        y_to_far(i).wait_send()

    loop(4, last)
    for i in range(2):
        pltpu.make_async_copy(a_loc.at[2 * cc + i], out_hbm.at[pl.ds(i * B, B), :], x_loc.at[i]).wait()


def solution(mesh):
    bf, f = jnp.bfloat16, jnp.float32
    dma = pltpu.SemaphoreType.DMA

    def step(x, gain, wq, wk, wv, wo):
        hbm = pl.BlockSpec(memory_space=pl.ANY)
        vmem = pl.BlockSpec(memory_space=pltpu.VMEM)
        return pl.pallas_call(
            _kernel,
            out_shape=jax.ShapeDtypeStruct(x.shape, bf),
            in_specs=[hbm, vmem, vmem, hbm, hbm, hbm, hbm],
            out_specs=hbm,
            scratch_shapes=[
                pltpu.VMEM((8, B, 1024), bf),
                pltpu.VMEM((4, B, 1024), bf),
                pltpu.VMEM((3, 4, 1024, 256), bf),
                pltpu.VMEM((1024, 1024), bf),
                pltpu.VMEM((8, 8, B, HEAD), bf),
                pltpu.VMEM((8, 8, HEAD + 16, B), bf),
                pltpu.VMEM((5, 8, B, HEAD), bf),
                pltpu.VMEM((B, 1024), bf),
                pltpu.VMEM((B, HEAD), f),
                pltpu.VMEM((B, HEAD), f),
                pltpu.VMEM((QUAD, B), f),
                pltpu.VMEM((QUAD, HEAD + 16, B), f),
                pltpu.VMEM((QUAD, B, B), f),
                pltpu.VMEM((QUAD, B), f),
                pltpu.VMEM((2, B, 1024), f),
                pltpu.VMEM((2, B, 1024), bf),
                pltpu.VMEM((2, 2, B // 2, 1024), bf),
                pltpu.VMEM((4, B // 2, 1024), bf),
                dma((3, 4, 3)), dma((3, 4, 4)), dma((3, 2, 2)),
                dma((2,)), dma((2,)), dma((2,)), dma((4,)), dma((4,)), dma((4,)), dma((4,)),
                dma((2,)), dma((2,)), dma((4,)), dma((4,)), dma((4,)), dma((2, 2)), dma((2,)),
            ],
            compiler_params=pltpu.CompilerParams(collective_id=0, has_side_effects=True, vmem_limit_bytes=67043328),
            name="layer",
        )(x, gain, _angles(), wq, wk, wv, wo)

    tokens, whole = P(("dp", "sp"), None), P("sp", None)
    return jax.shard_map(
        step,
        mesh=mesh,
        in_specs=(tokens, P(None), whole, whole, whole, whole),
        out_specs=tokens,
        check_vma=False,
    )
```

```python
import functools

import jax
import jax.numpy as jnp
import numpy as np
from jax import lax
from jax.experimental import pallas as pl
from jax.experimental.pallas import tpu as pltpu
from jax.sharding import PartitionSpec as P

HEAD = 128
THETA = 10000
NEG = -1e30
HIDDEN = 2 * NEG
LOG2E = 1.4426950408889634
B = 512
QUAD = 4
MESH = pl.DeviceIdType.MESH


def _dot(a, b, ca, cb):
    return lax.dot_general(a, b, (((ca,), (cb,)), ((), ())), preferred_element_type=jnp.float32)


def _angles():
    freq = np.float64(THETA) ** (-np.arange(64) / 64)
    freq = np.concatenate([freq, freq])
    sign = np.concatenate([-np.ones(64), np.ones(64)])
    coarse = 64 * np.arange(64)[:, None] * freq
    fine = np.arange(64)[:, None] * freq
    out = np.stack([np.cos(coarse), np.sin(coarse) * sign, np.cos(fine), np.sin(fine) * sign])
    return jnp.asarray(out.astype(np.float32))


def _kernel(x_hbm, gain_ref, ang_ref, wq_hbm, wk_hbm, wv_hbm, wo_hbm, out_hbm,
            xs, a_loc, w, wo, k_s, vt_s, q_s, a_far, cos_s, sin_s, top_s, mix_s, s_s, peak_s, y_own, from_mate, from_far, half_in,
            w_send, w_recv, w_fwd, x_loc, x_mate_send, x_mate, x_send, x_dir, x_fwd_send, x_fwd,
            mate_send, mate_recv, half_send, half_recv, far_send, far_recv, misc):
    me = lax.axis_index("sp")
    y = lax.axis_index("dp")
    xx, cc = lax.div(me, 2), lax.rem(me, 2)
    mate = 2 * xx + 1 - cc
    far = 2 * (1 - xx) + cc
    far0 = 2 * (1 - xx)
    weights = (wk_hbm, wv_hbm, wq_hbm)
    rows = B // 2
    depth = 256

    barrier = pltpu.get_barrier_semaphore()
    for peer in (mate, far, 2 * (1 - xx) + 1 - cc):
        pl.semaphore_signal(barrier, inc=1, device_id={"dp": y, "sp": peer}, device_id_type=MESH)
    pl.semaphore_signal(barrier, inc=1, device_id={"dp": 1 - y, "sp": me}, device_id_type=MESH)
    pl.semaphore_wait(barrier, 4)

    def remote(src, dst, send, recv, sp, dp=y):
        return pltpu.make_async_remote_copy(src_ref=src, dst_ref=dst, send_sem=send, recv_sem=recv, device_id={"dp": dp, "sp": sp},
                                            device_id_type=MESH)

    def w_place(m, hp, sender):
        return w.at[m, hp, pl.ds(pl.multiple_of(sender * depth, depth), depth), :]

    def w_columns(m, hp, owner):
        return weights[m].at[:, pl.ds(pl.multiple_of(owner * 1024 + hp * 256, 256), 256)]

    def w_to(m, hp, owner, n):
        return remote(w_columns(m, hp, owner), w_place(m, hp, me), w_send.at[m, hp, n], w_recv.at[m, hp, me], owner)

    def w_from(m, hp, sender):
        return remote(w_place(m, hp, sender), w_place(m, hp, sender), misc.at[0], w_recv.at[m, hp, sender], sender)

    def w_on(m, hp, n):
        place = w_place(m, hp, far0 + n)
        return remote(place, place, w_fwd.at[m, lax.div(hp, 2), n], w_recv.at[m, hp, far0 + n], me, 1 - y)

    def w_own(m, hp):
        return pltpu.make_async_copy(w_columns(m, hp, me), w_place(m, hp, me), w_recv.at[m, hp, me])

    def x_own(i):
        return pltpu.make_async_copy(x_hbm.at[pl.ds(i * B, B), :], xs.at[2 * me + i], x_loc.at[i])

    def x_to_mate(i):
        return remote(x_hbm.at[pl.ds(i * B, B), :], xs.at[2 * me + i], x_mate_send.at[i], x_mate.at[i], mate)

    def x_from_mate(i):
        return remote(xs.at[2 * mate + i], xs.at[2 * mate + i], misc.at[0], x_mate.at[i], mate)

    def x_half(b, c):
        return xs.at[b, pl.ds(pl.multiple_of(c * rows, rows), rows), :]

    def x_to_far(i):
        return remote(x_half(4 * xx + i, cc), x_half(4 * xx + i, cc), x_send.at[i], x_dir.at[i], far)

    def x_from_far(i):
        place = x_half(4 * (1 - xx) + i, cc)
        return remote(place, place, misc.at[0], x_dir.at[i], far)

    def x_on(i):
        place = x_half(4 * (1 - xx) + i, cc)
        return remote(place, place, x_fwd_send.at[i], x_fwd.at[i], mate)

    def x_on_from(i):
        place = x_half(4 * (1 - xx) + i, 1 - cc)
        return remote(place, place, misc.at[0], x_fwd.at[i], mate)

    def y_to_mate(i):
        return remote(a_loc.at[i], from_mate.at[lax.rem(i, 2)], mate_send.at[lax.rem(i, 2)], mate_recv.at[lax.rem(i, 2)], mate)

    def y_from_mate(i):
        return remote(from_mate.at[i], from_mate.at[i], misc.at[0], mate_recv.at[i], mate)

    def half_to_mate(i):
        return remote(x_half(4 * (1 - xx) + i, 1 - cc), half_in.at[i], half_send.at[i], half_recv.at[i], mate)

    def half_from_mate(i):
        return remote(half_in.at[i], half_in.at[i], misc.at[0], half_recv.at[i], mate)

    def y_to_far(i):
        owner = 2 * (1 - xx) + lax.div(i, 2)
        return remote(x_half(4 * (1 - xx) + i, cc), from_far.at[lax.rem(i, 2), cc], far_send.at[i], far_recv.at[lax.rem(i, 2), cc], owner)

    def y_from_far(i, c):
        return remote(from_far.at[i, c], from_far.at[i, c], misc.at[0], far_recv.at[i, c], far0 + c)

    def loop(n, body):
        lax.fori_loop(0, n, lambda i, _: (body(i), None)[1], None)

    def hp_at(it):
        return 2 * lax.div(it, 2) + jnp.where(lax.rem(it, 2) == 0, y, 1 - y)

    def crossing(g):
        if isinstance(g, int) and g < 6:
            return [w_to(g % 3, hp_at(2 * (g // 3)), far0 + (cc if n == 1 else 1 - cc), n) for n in (1, 2)]
        return [x_to_far(g - 6)]

    def cross(g):
        for copy in crossing(g - 2):
            copy.wait_send()
        for copy in crossing(g):
            copy.start()

    for g in range(2):
        for copy in crossing(g):
            copy.start()
    for i in range(2):
        x_own(i).start()
        x_to_mate(i).start()
    for it in range(4):
        hp = hp_at(it)
        for m in range(3):
            w_own(m, hp).start()
            w_to(m, hp, mate, 0).start()
    wo_copy = pltpu.make_async_copy(wo_hbm, wo, misc.at[1])
    wo_copy.start()

    def arrive(m, hp, onward):
        for n in range(2):
            w_from(m, hp, far0 + n).wait_recv()
            if onward:
                w_on(m, hp, n).start()

    arrive(0, hp_at(0), True)
    cross(2)
    for i in range(2):
        x_own(i).wait()
    for i in range(2):
        x_from_mate(i).wait_recv()

    gain = gain_ref[...].astype(jnp.float32)[None, :]

    def norm(src, dst):
        def part(r):
            here = pl.ds(pl.multiple_of(r * 256, 256), 256)
            wide = src[here, :].astype(jnp.float32)
            scale = lax.rsqrt(jnp.mean(wide * wide, -1, keepdims=True) + 1e-6)
            dst[here, :] = (wide * scale * gain).astype(jnp.bfloat16)

        loop(B // 256, part)

    def turn_table(b):
        for r in range(B // 64):
            here = pl.ds(r * 64, 64)
            at = pl.ds(b * (B // 64) + r, 1)
            ch, sh, cf, sf = ang_ref[0, at, :], ang_ref[1, at, :], ang_ref[2], ang_ref[3]
            cos_s[here, :] = ch * cf - sh * sf
            sin_s[here, :] = sh * cf + ch * sf

    def turned(t):
        t = t.astype(jnp.float32)
        return (t * cos_s[...] + pltpu.roll(t, 64, 1) * sin_s[...]).astype(jnp.bfloat16)

    def project_one(a, m, hp, b, slot):
        t = _dot(a[...], w[m, hp], 1, 0).astype(jnp.bfloat16)
        for i in range(2):
            part = t[:, i * HEAD : (i + 1) * HEAD]
            if m == 0:
                k_s[b, 2 * hp + i] = turned(part)
            elif m == 1:
                vt_s[b, 2 * hp + i, 0:HEAD, :] = part.T
            else:
                q_s[slot, 2 * hp + i] = turned(part)

    def project(a, hp, b, slot):
        for m in range(3):
            project_one(a, m, hp, b, slot)

    e = HEAD**-0.5 * LOG2E

    def scores(j, slot, h, n):
        s = _dot(k_s[j, h], q_s[slot, h], 1, 1)
        peak_s[n : n + 1, :] = s.max(axis=0, keepdims=True)
        s_s[n] = s

    def attend(qb, slot, quad, lo, hi, after, *, diagonal=True, state=0, fresh=True, first=True, final=True):
        @pl.when(fresh)
        def _():
            top_s[state] = jnp.full(top_s.shape[1:], NEG, jnp.float32)
            mix_s[state] = jnp.zeros(mix_s.shape[1:], jnp.float32)

        @pl.when(first)
        def _():
            for n in range(QUAD):
                scores(lo, slot, quad * QUAD + n, n)

        def whole(j):
            more = diagonal | (j + 1 < hi)
            key, where, which = jnp.where(more, j + 1, after[0]), jnp.where(more, slot, after[1]), jnp.where(more, quad, after[2])
            for n in range(QUAD):
                old = top_s[state, n : n + 1, :]
                top = jnp.maximum(old, peak_s[n : n + 1, :])
                top_s[state, n : n + 1, :] = top
                p = jnp.exp2((s_s[n] - top) * e).astype(jnp.bfloat16)
                scores(key, where, which * QUAD + n, n)
                mix_s[state, n] = mix_s[state, n] * jnp.exp2((old - top) * e) + _dot(vt_s[j, quad * QUAD + n], p, 1, 0)

        def two(t):
            whole(lo + 2 * t)
            whole(lo + 2 * t + 1)

        loop(lax.div(hi - lo, 2), two)

        @pl.when(lax.rem(hi - lo, 2) == 1)
        def _():
            whole(hi - 1)

        @pl.when(diagonal)
        def _():
            half = B // 2
            ok = lax.broadcasted_iota(jnp.int32, (half, half), 1) >= lax.broadcasted_iota(jnp.int32, (half, half), 0)
            for n in range(QUAD):
                h = quad * QUAD + n
                for at in (0, half):
                    cols = slice(at, at + half)
                    parts = [s_s[n, 0:half, cols], jnp.where(ok, s_s[n, half:B, cols], HIDDEN)] if at else [jnp.where(ok, s_s[n, 0:half, cols], HIDDEN)]
                    old = top_s[state, n : n + 1, cols]
                    top = old
                    for part in parts:
                        top = jnp.maximum(top, part.max(axis=0, keepdims=True))
                    top_s[state, n : n + 1, cols] = top
                    p = jnp.concatenate([jnp.exp2((part - top) * e).astype(jnp.bfloat16) for part in parts], axis=0)
                    mix_s[state, n, :, cols] = (mix_s[state, n, :, cols] * jnp.exp2((old - top) * e)
                                                + _dot(vt_s[qb, h, :, 0 : at + half], p, 1, 0))
                scores(after[0], after[1], after[2] * QUAD + n, n)

        @pl.when(final)
        def _():
            for n in range(QUAD):
                out = mix_s[state, n, 0:HEAD, :] * (1 / mix_s[state, n, HEAD : HEAD + 1, :])
                q_s[slot, quad * QUAD + n] = out.T.astype(jnp.bfloat16)

    def combine(i):
        def part(r):
            here = pl.ds(pl.multiple_of(cc * rows + r * 64, 64), 64)
            at = pl.ds(pl.multiple_of(r * 64, 64), 64)
            b = 4 * (1 - xx) + i
            xs[b, here, :] = (xs[b, here, :].astype(jnp.float32) + half_in[i, at, :].astype(jnp.float32)).astype(jnp.bfloat16)

        loop(rows // 64, part)

    vt_s[:, :, HEAD:, :] = jnp.ones(vt_s.shape[:2] + (vt_s.shape[2] - HEAD, B), jnp.bfloat16)
    loop(4, lambda i: norm(xs.at[4 * xx + i], a_loc.at[i]))

    def pair(it):
        hp = hp_at(it)
        for m in range(3):
            w_own(m, hp).wait()
            w_from(m, hp, mate).wait_recv()

        @pl.when(it == 0)
        def _():
            for m in (1, 2):
                arrive(m, hp, True)
                cross(2 + m)

        @pl.when(it == 1)
        def _():
            arrive(0, hp_at(2), True)
            cross(5)
            for m in range(3):
                arrive(m, hp, False)

        @pl.when(it == 2)
        def _():
            for m in (1, 2):
                arrive(m, hp, True)
                cross(5 + m)

        @pl.when(it == 3)
        def _():
            for m in range(3):
                arrive(m, hp, False)

        def tokens(t):
            for i in (2 * t, 2 * t + 1):
                turn_table(4 * xx + i)
                project(a_loc.at[i], hp, 4 * xx + i, i)

        loop(2, tokens)

        @pl.when((it == 1) | ((it == 3) & (xx == 1)))
        def _():
            quad = lax.div(it, 2)
            short = it == 3
            attend(4 * xx + 3, 3, quad, 4 * xx, 4 * xx + 3 - quad, (jnp.where(short, 6, 0), 3, quad), diagonal=jnp.logical_not(short),
                   state=xx * (1 + quad), final=xx == 0)

    loop(4, pair)
    wo_copy.wait()

    first = 2 * (1 - xx)

    def forward_x(i):
        x_from_far(i).wait_recv()
        x_on(i).start()

    @pl.when(xx == 1)
    def _():
        forward_x(0)
        attend(7, 3, 1, 6, 7, (0, 4, 0), state=2, fresh=False, first=False, final=False)

    def blocks(s):
        i = s - first
        away = (i >= 0) & (i < 4)
        qb = jnp.where(xx == 1, s, jnp.where(s < 2, s, jnp.where(s < 6, s + 2, s - 4)))
        here = qb - 4 * xx
        return i, away, qb, here, jnp.where(away, 4, here)

    def step(s):
        @pl.when((s == 1) | (s == 2))
        def _():
            cross(s + 7)

        i, away, qb, here, slot = blocks(s)
        begun = s == 7
        next_slot = blocks(s + 1)[-1]

        @pl.when(away)
        def _():
            x_on(i).wait_send()
            x_on_from(i).wait_recv()
            norm(xs.at[qb], a_far)
            turn_table(qb)
            for hp in range(4):
                project(a_far, hp, qb, 4)

        def quad(n):
            resume = begun & (xx == 1)

            @pl.when(jnp.logical_not(begun & (xx == 0) & (n == 0)))
            def _():
                attend(qb, slot, n, 0, jnp.where(resume, 4, qb),
                       (0, jnp.where(n == 0, slot, next_slot), jnp.where(n == 0, 1, jnp.where((s == 6) & (xx == 0), 1, 0))),
                       diagonal=jnp.logical_not(resume), state=jnp.where(resume, 1 + n, 0), fresh=jnp.logical_not(resume),
                       first=(n == 0) & (away | (s == 0)))

            @pl.when((n == 0) & (i >= 1) & (i < 5))
            def _():
                half_from_mate(i - 1).wait_recv()
                combine(i - 1)
                y_to_far(i - 1).start()

        loop(8 // QUAD, quad)

        @pl.when((i >= -1) & (i < 3))
        def _():
            forward_x(i + 1)

        own = jnp.logical_not(away) & (lax.div(here, 2) == cc)

        def output(store):
            seen = jnp.concatenate([q_s[slot, h] for h in range(8)], axis=1)
            for n in range(4):
                cols = slice(n * 256, n * 256 + 256)
                store(cols, _dot(seen, wo[:, cols], 1, 0))

        @pl.when(own)
        def _():
            def store(cols, r):
                y_own[lax.rem(here, 2), :, cols] = r

            output(store)

        @pl.when(away)
        def _():
            def store(cols, r):
                xs[qb, :, cols] = r.astype(jnp.bfloat16)

            output(store)

        @pl.when(jnp.logical_not(own | away))
        def _():
            def store(cols, r):
                a_loc[here, :, cols] = r.astype(jnp.bfloat16)

            output(store)

        @pl.when(away)
        def _():
            half_to_mate(i).start()

        @pl.when(jnp.logical_not(own | away))
        def _():
            y_to_mate(here).start()

    loop(8, step)

    for i in range(2):
        y_from_mate(i).wait_recv()
        for c in range(2):
            y_from_far(i, c).wait_recv()
            base = c * rows

            def part(r):
                here = pl.ds(pl.multiple_of(base + r * 32, 32), 32)
                at = pl.ds(pl.multiple_of(r * 32, 32), 32)
                f = jnp.float32
                total = y_own[i, here, :] + from_mate[i, here, :].astype(f) + from_far[i, c, at, :].astype(f)
                a_loc[2 * cc + i, here, :] = (xs[2 * me + i, here, :].astype(f) + total).astype(jnp.bfloat16)

            loop(rows // 32, part)
        pltpu.make_async_copy(a_loc.at[2 * cc + i], out_hbm.at[pl.ds(i * B, B), :], x_loc.at[i]).start()

    for i in range(2):
        x_to_mate(i).wait_send()
        y_to_mate(2 * (1 - cc) + i).wait_send()
    for it in range(4):
        hp = hp_at(it)
        for m in range(3):
            w_to(m, hp, mate, 0).wait_send()
            if it % 2 == 0:
                for n in range(2):
                    w_on(m, hp, n).wait_send()

    for i in (2, 3):
        x_to_far(i).wait_send()

    def last(i):
        half_to_mate(i).wait_send()
        y_to_far(i).wait_send()

    loop(4, last)
    for i in range(2):
        pltpu.make_async_copy(a_loc.at[2 * cc + i], out_hbm.at[pl.ds(i * B, B), :], x_loc.at[i]).wait()


def solution(mesh):
    bf, f = jnp.bfloat16, jnp.float32
    dma = pltpu.SemaphoreType.DMA

    def step(x, gain, wq, wk, wv, wo):
        hbm = pl.BlockSpec(memory_space=pl.ANY)
        vmem = pl.BlockSpec(memory_space=pltpu.VMEM)
        return pl.pallas_call(
            _kernel,
            out_shape=jax.ShapeDtypeStruct(x.shape, bf),
            in_specs=[hbm, vmem, vmem, hbm, hbm, hbm, hbm],
            out_specs=hbm,
            scratch_shapes=[
                pltpu.VMEM((8, B, 1024), bf),
                pltpu.VMEM((4, B, 1024), bf),
                pltpu.VMEM((3, 4, 1024, 256), bf),
                pltpu.VMEM((1024, 1024), bf),
                pltpu.VMEM((8, 8, B, HEAD), bf),
                pltpu.VMEM((8, 8, HEAD + 16, B), bf),
                pltpu.VMEM((5, 8, B, HEAD), bf),
                pltpu.VMEM((B, 1024), bf),
                pltpu.VMEM((B, HEAD), f),
                pltpu.VMEM((B, HEAD), f),
                pltpu.VMEM((3, QUAD, B), f),
                pltpu.VMEM((3, QUAD, HEAD + 16, B), f),
                pltpu.VMEM((QUAD, B, B), f),
                pltpu.VMEM((QUAD, B), f),
                pltpu.VMEM((2, B, 1024), f),
                pltpu.VMEM((2, B, 1024), bf),
                pltpu.VMEM((2, 2, B // 2, 1024), bf),
                pltpu.VMEM((4, B // 2, 1024), bf),
                dma((3, 4, 3)), dma((3, 4, 4)), dma((3, 2, 2)),
                dma((2,)), dma((2,)), dma((2,)), dma((4,)), dma((4,)), dma((4,)), dma((4,)),
                dma((2,)), dma((2,)), dma((4,)), dma((4,)), dma((4,)), dma((2, 2)), dma((2,)),
            ],
            compiler_params=pltpu.CompilerParams(collective_id=0, has_side_effects=True, vmem_limit_bytes=67043328),
            name="layer",
        )(x, gain, _angles(), wq, wk, wv, wo)

    tokens, whole = P(("dp", "sp"), None), P("sp", None)
    return jax.shard_map(
        step,
        mesh=mesh,
        in_specs=(tokens, P(None), whole, whole, whole, whole),
        out_specs=tokens,
        check_vma=False,
    )
```

```python
import functools

import jax
import jax.numpy as jnp
import numpy as np
from jax import lax
from jax.experimental import pallas as pl
from jax.experimental.pallas import tpu as pltpu
from jax.sharding import PartitionSpec as P

HEAD = 128
THETA = 10000
NEG = -1e30
HIDDEN = 2 * NEG
LOG2E = 1.4426950408889634
B = 512
QUAD = 4
MESH = pl.DeviceIdType.MESH


def _dot(a, b, ca, cb):
    return lax.dot_general(a, b, (((ca,), (cb,)), ((), ())), preferred_element_type=jnp.float32)


def _angles():
    freq = np.float64(THETA) ** (-np.arange(64) / 64)
    freq = np.concatenate([freq, freq])
    sign = np.concatenate([-np.ones(64), np.ones(64)])
    coarse = 64 * np.arange(64)[:, None] * freq
    fine = np.arange(64)[:, None] * freq
    out = np.stack([np.cos(coarse), np.sin(coarse) * sign, np.cos(fine), np.sin(fine) * sign])
    return jnp.asarray(out.astype(np.float32))


def _kernel(x_hbm, gain_ref, ang_ref, wq_hbm, wk_hbm, wv_hbm, wo_hbm, out_hbm,
            xs, a_loc, w, wo, k_s, vt_s, q_s, a_far, cos_s, sin_s, top_s, mix_s, s_s, peak_s, y_own, from_mate, from_far, half_in,
            w_send, w_recv, w_fwd, x_loc, x_mate_send, x_mate, x_send, x_dir, x_fwd_send, x_fwd,
            mate_send, mate_recv, half_send, half_recv, far_send, far_recv, misc):
    me = lax.axis_index("sp")
    y = lax.axis_index("dp")
    xx, cc = lax.div(me, 2), lax.rem(me, 2)
    mate = 2 * xx + 1 - cc
    far = 2 * (1 - xx) + cc
    far0 = 2 * (1 - xx)
    weights = (wk_hbm, wv_hbm, wq_hbm)
    rows = B // 2
    depth = 256

    barrier = pltpu.get_barrier_semaphore()
    for peer in (mate, far, 2 * (1 - xx) + 1 - cc):
        pl.semaphore_signal(barrier, inc=1, device_id={"dp": y, "sp": peer}, device_id_type=MESH)
    pl.semaphore_signal(barrier, inc=1, device_id={"dp": 1 - y, "sp": me}, device_id_type=MESH)
    pl.semaphore_wait(barrier, 4)

    def remote(src, dst, send, recv, sp, dp=y):
        return pltpu.make_async_remote_copy(src_ref=src, dst_ref=dst, send_sem=send, recv_sem=recv, device_id={"dp": dp, "sp": sp},
                                            device_id_type=MESH)

    def w_place(m, hp, sender):
        return w.at[m, hp, pl.ds(pl.multiple_of(sender * depth, depth), depth), :]

    def w_columns(m, hp, owner):
        return weights[m].at[:, pl.ds(pl.multiple_of(owner * 1024 + hp * 256, 256), 256)]

    def w_to(m, hp, owner, n):
        return remote(w_columns(m, hp, owner), w_place(m, hp, me), w_send.at[m, hp, n], w_recv.at[m, hp, me], owner)

    def w_from(m, hp, sender):
        return remote(w_place(m, hp, sender), w_place(m, hp, sender), misc.at[0], w_recv.at[m, hp, sender], sender)

    def w_on(m, hp, n):
        place = w_place(m, hp, far0 + n)
        return remote(place, place, w_fwd.at[m, lax.div(hp, 2), n], w_recv.at[m, hp, far0 + n], me, 1 - y)

    def w_own(m, hp):
        return pltpu.make_async_copy(w_columns(m, hp, me), w_place(m, hp, me), w_recv.at[m, hp, me])

    def x_own(i):
        return pltpu.make_async_copy(x_hbm.at[pl.ds(i * B, B), :], xs.at[2 * me + i], x_loc.at[i])

    def x_to_mate(i):
        return remote(x_hbm.at[pl.ds(i * B, B), :], xs.at[2 * me + i], x_mate_send.at[i], x_mate.at[i], mate)

    def x_from_mate(i):
        return remote(xs.at[2 * mate + i], xs.at[2 * mate + i], misc.at[0], x_mate.at[i], mate)

    def x_half(b, c):
        return xs.at[b, pl.ds(pl.multiple_of(c * rows, rows), rows), :]

    def x_to_far(i):
        return remote(x_half(4 * xx + i, cc), x_half(4 * xx + i, cc), x_send.at[i], x_dir.at[i], far)

    def x_from_far(i):
        place = x_half(4 * (1 - xx) + i, cc)
        return remote(place, place, misc.at[0], x_dir.at[i], far)

    def x_on(i):
        place = x_half(4 * (1 - xx) + i, cc)
        return remote(place, place, x_fwd_send.at[i], x_fwd.at[i], mate)

    def x_on_from(i):
        place = x_half(4 * (1 - xx) + i, 1 - cc)
        return remote(place, place, misc.at[0], x_fwd.at[i], mate)

    def y_to_mate(i):
        return remote(a_loc.at[i], from_mate.at[lax.rem(i, 2)], mate_send.at[lax.rem(i, 2)], mate_recv.at[lax.rem(i, 2)], mate)

    def y_from_mate(i):
        return remote(from_mate.at[i], from_mate.at[i], misc.at[0], mate_recv.at[i], mate)

    def half_to_mate(i):
        return remote(x_half(4 * (1 - xx) + i, 1 - cc), half_in.at[i], half_send.at[i], half_recv.at[i], mate)

    def half_from_mate(i):
        return remote(half_in.at[i], half_in.at[i], misc.at[0], half_recv.at[i], mate)

    def y_to_far(i):
        owner = 2 * (1 - xx) + lax.div(i, 2)
        return remote(x_half(4 * (1 - xx) + i, cc), from_far.at[lax.rem(i, 2), cc], far_send.at[i], far_recv.at[lax.rem(i, 2), cc], owner)

    def y_from_far(i, c):
        return remote(from_far.at[i, c], from_far.at[i, c], misc.at[0], far_recv.at[i, c], far0 + c)

    def loop(n, body):
        lax.fori_loop(0, n, lambda i, _: (body(i), None)[1], None)

    def hp_at(it):
        return 2 * lax.div(it, 2) + jnp.where(lax.rem(it, 2) == 0, y, 1 - y)

    def crossing(g):
        if isinstance(g, int) and g < 6:
            return [w_to(g % 3, hp_at(2 * (g // 3)), far0 + (cc if n == 1 else 1 - cc), n) for n in (1, 2)]
        return [x_to_far(g - 6)]

    def cross(g):
        for copy in crossing(g - 2):
            copy.wait_send()
        for copy in crossing(g):
            copy.start()

    for g in range(2):
        for copy in crossing(g):
            copy.start()
    for i in range(2):
        x_own(i).start()
        x_to_mate(i).start()
    for it in range(4):
        hp = hp_at(it)
        for m in range(3):
            w_own(m, hp).start()
            w_to(m, hp, mate, 0).start()
    wo_copy = pltpu.make_async_copy(wo_hbm, wo, misc.at[1])
    wo_copy.start()

    def arrive(m, hp, onward):
        for n in range(2):
            w_from(m, hp, far0 + n).wait_recv()
            if onward:
                w_on(m, hp, n).start()

    arrive(0, hp_at(0), True)
    cross(2)
    for i in range(2):
        x_own(i).wait()
    for i in range(2):
        x_from_mate(i).wait_recv()

    gain = gain_ref[...].astype(jnp.float32)[None, :]

    def norm(src, dst):
        def part(r):
            here = pl.ds(pl.multiple_of(r * 256, 256), 256)
            wide = src[here, :].astype(jnp.float32)
            scale = lax.rsqrt(jnp.mean(wide * wide, -1, keepdims=True) + 1e-6)
            dst[here, :] = (wide * scale * gain).astype(jnp.bfloat16)

        loop(B // 256, part)

    def turn_table(b):
        for r in range(B // 64):
            here = pl.ds(r * 64, 64)
            at = pl.ds(b * (B // 64) + r, 1)
            ch, sh, cf, sf = ang_ref[0, at, :], ang_ref[1, at, :], ang_ref[2], ang_ref[3]
            cos_s[here, :] = ch * cf - sh * sf
            sin_s[here, :] = sh * cf + ch * sf

    def turned(t):
        t = t.astype(jnp.float32)
        return (t * cos_s[...] + pltpu.roll(t, 64, 1) * sin_s[...]).astype(jnp.bfloat16)

    def project_one(a, m, hp, b, slot):
        t = _dot(a[...], w[m, hp], 1, 0).astype(jnp.bfloat16)
        for i in range(2):
            part = t[:, i * HEAD : (i + 1) * HEAD]
            if m == 0:
                k_s[b, 2 * hp + i] = turned(part)
            elif m == 1:
                vt_s[b, 2 * hp + i, 0:HEAD, :] = part.T
            else:
                q_s[slot, 2 * hp + i] = turned(part)

    def project(a, hp, b, slot):
        for m in range(3):
            project_one(a, m, hp, b, slot)

    e = HEAD**-0.5 * LOG2E

    def scores(j, slot, h, n):
        s = _dot(k_s[j, h], q_s[slot, h], 1, 1)
        peak_s[n : n + 1, :] = s.max(axis=0, keepdims=True)
        s_s[n] = s

    def attend(qb, slot, quad, lo, hi, after, *, diagonal=True, state=0, first=True, final=True):
        @pl.when(first)
        def _():
            for n in range(QUAD):
                scores(lo, slot, quad * QUAD + n, n)

        def whole(j):
            more = diagonal | (j + 1 < hi)
            key, where, which = jnp.where(more, j + 1, after[0]), jnp.where(more, slot, after[1]), jnp.where(more, quad, after[2])
            for n in range(QUAD):
                old = top_s[state, n : n + 1, :]
                top = jnp.maximum(old, peak_s[n : n + 1, :])
                top_s[state, n : n + 1, :] = top
                p = jnp.exp2((s_s[n] - top) * e).astype(jnp.bfloat16)
                scores(key, where, which * QUAD + n, n)
                mix_s[state, n] = mix_s[state, n] * jnp.exp2((old - top) * e) + _dot(vt_s[j, quad * QUAD + n], p, 1, 0)

        def finish():
            for n in range(QUAD):
                out = mix_s[state, n, 0:HEAD, :] * (1 / mix_s[state, n, HEAD : HEAD + 1, :])
                q_s[slot, quad * QUAD + n] = out.T.astype(jnp.bfloat16)
                mix_s[state, n] = jnp.zeros(mix_s.shape[2:], jnp.float32)
            top_s[state] = jnp.full(top_s.shape[1:], NEG, jnp.float32)

        def two(t):
            whole(lo + 2 * t)
            whole(lo + 2 * t + 1)

        loop(lax.div(hi - lo, 2), two)

        @pl.when(lax.rem(hi - lo, 2) == 1)
        def _():
            whole(hi - 1)

        @pl.when(diagonal)
        def _():
            half = B // 2
            ok = lax.broadcasted_iota(jnp.int32, (half, half), 1) >= lax.broadcasted_iota(jnp.int32, (half, half), 0)
            for n in range(QUAD):
                h = quad * QUAD + n
                for at in (0, half):
                    cols = slice(at, at + half)
                    parts = [s_s[n, 0:half, cols], jnp.where(ok, s_s[n, half:B, cols], HIDDEN)] if at else [jnp.where(ok, s_s[n, 0:half, cols], HIDDEN)]
                    old = top_s[state, n : n + 1, cols]
                    top = old
                    for part in parts:
                        top = jnp.maximum(top, part.max(axis=0, keepdims=True))
                    top_s[state, n : n + 1, cols] = top
                    p = jnp.concatenate([jnp.exp2((part - top) * e).astype(jnp.bfloat16) for part in parts], axis=0)
                    mix_s[state, n, :, cols] = (mix_s[state, n, :, cols] * jnp.exp2((old - top) * e)
                                                + _dot(vt_s[qb, h, :, 0 : at + half], p, 1, 0))
                scores(after[0], after[1], after[2] * QUAD + n, n)
            if final is True:
                finish()

        if final is not True:
            pl.when(final)(finish)
        elif diagonal is not True:
            pl.when(jnp.logical_not(diagonal))(finish)

    def combine(i):
        def part(r):
            here = pl.ds(pl.multiple_of(cc * rows + r * 64, 64), 64)
            at = pl.ds(pl.multiple_of(r * 64, 64), 64)
            b = 4 * (1 - xx) + i
            xs[b, here, :] = (xs[b, here, :].astype(jnp.float32) + half_in[i, at, :].astype(jnp.float32)).astype(jnp.bfloat16)

        loop(rows // 64, part)

    top_s[...] = jnp.full(top_s.shape, NEG, jnp.float32)
    mix_s[...] = jnp.zeros(mix_s.shape, jnp.float32)
    vt_s[:, :, HEAD:, :] = jnp.ones(vt_s.shape[:2] + (vt_s.shape[2] - HEAD, B), jnp.bfloat16)
    loop(4, lambda i: norm(xs.at[4 * xx + i], a_loc.at[i]))

    def pair(it):
        hp = hp_at(it)
        for m in range(3):
            w_own(m, hp).wait()
            w_from(m, hp, mate).wait_recv()

        @pl.when(it == 0)
        def _():
            for m in (1, 2):
                arrive(m, hp, True)
                cross(2 + m)

        @pl.when(it == 1)
        def _():
            arrive(0, hp_at(2), True)
            cross(5)
            for m in range(3):
                arrive(m, hp, False)

        @pl.when(it == 2)
        def _():
            arrive(2, hp, True)
            cross(7)

        @pl.when(it == 3)
        def _():
            for m in range(3):
                arrive(m, hp, False)

        def tokens(t):
            for i in (2 * t, 2 * t + 1):
                turn_table(4 * xx + i)
                project(a_loc.at[i], hp, 4 * xx + i, i)

        loop(2, tokens)

        @pl.when(it == 1)
        def _():
            arrive(1, hp_at(2), True)
            cross(6)

        @pl.when((it == 1) | ((it == 3) & (xx == 1)))
        def _():
            quad = lax.div(it, 2)
            short = it == 3
            attend(4 * xx + 3, 3, quad, 4 * xx, 4 * xx + 3 - quad, (jnp.where(short, 6, 0), 3, quad), diagonal=jnp.logical_not(short),
                   state=xx * (1 + quad), final=xx == 0)

    loop(4, pair)
    wo_copy.wait()

    first = 2 * (1 - xx)

    def forward_x(i):
        x_from_far(i).wait_recv()
        x_on(i).start()

    @pl.when(xx == 1)
    def _():
        forward_x(0)
        attend(7, 3, 1, 6, 7, (0, 4, 0), state=2, first=False, final=False)

    def blocks(s):
        i = s - first
        away = (i >= 0) & (i < 4)
        qb = jnp.where(xx == 1, s, jnp.where(s < 2, s, jnp.where(s < 6, s + 2, s - 4)))
        here = qb - 4 * xx
        return i, away, qb, here, jnp.where(away, 4, here)

    def step(s):
        @pl.when((s == 1) | (s == 2))
        def _():
            cross(s + 7)

        i, away, qb, here, slot = blocks(s)
        begun = s == 7
        next_slot = blocks(s + 1)[-1]

        @pl.when(away)
        def _():
            x_on(i).wait_send()
            x_on_from(i).wait_recv()
            norm(xs.at[qb], a_far)
            turn_table(qb)
            for hp in range(4):
                project(a_far, hp, qb, 4)

        def quad(n):
            resume = begun & (xx == 1)

            @pl.when(jnp.logical_not(begun & (xx == 0) & (n == 0)))
            def _():
                attend(qb, slot, n, 0, jnp.where(resume, 4, qb),
                       (0, jnp.where(n == 0, slot, next_slot), jnp.where(n == 0, 1, jnp.where((s == 6) & (xx == 0), 1, 0))),
                       diagonal=jnp.logical_not(resume), state=jnp.where(resume, 1 + n, 0), first=(n == 0) & (away | (s == 0)))

            @pl.when((n == 0) & (i >= 1) & (i < 5))
            def _():
                half_from_mate(i - 1).wait_recv()
                combine(i - 1)
                y_to_far(i - 1).start()

        loop(8 // QUAD, quad)

        @pl.when((i >= -1) & (i < 3))
        def _():
            forward_x(i + 1)

        own = jnp.logical_not(away) & (lax.div(here, 2) == cc)

        def output(store):
            seen = jnp.concatenate([q_s[slot, h] for h in range(8)], axis=1)
            for n in range(4):
                cols = slice(n * 256, n * 256 + 256)
                store(cols, _dot(seen, wo[:, cols], 1, 0))

        @pl.when(own)
        def _():
            def store(cols, r):
                y_own[lax.rem(here, 2), :, cols] = r

            output(store)

        @pl.when(away)
        def _():
            def store(cols, r):
                xs[qb, :, cols] = r.astype(jnp.bfloat16)

            output(store)

        @pl.when(jnp.logical_not(own | away))
        def _():
            def store(cols, r):
                a_loc[here, :, cols] = r.astype(jnp.bfloat16)

            output(store)

        @pl.when(away)
        def _():
            half_to_mate(i).start()

        @pl.when(jnp.logical_not(own | away))
        def _():
            y_to_mate(here).start()

    loop(8, step)

    for i in range(2):
        y_from_mate(i).wait_recv()
        for c in range(2):
            y_from_far(i, c).wait_recv()
            base = c * rows

            def part(r):
                here = pl.ds(pl.multiple_of(base + r * 32, 32), 32)
                at = pl.ds(pl.multiple_of(r * 32, 32), 32)
                f = jnp.float32
                total = y_own[i, here, :] + from_mate[i, here, :].astype(f) + from_far[i, c, at, :].astype(f)
                a_loc[2 * cc + i, here, :] = (xs[2 * me + i, here, :].astype(f) + total).astype(jnp.bfloat16)

            loop(rows // 32, part)
        pltpu.make_async_copy(a_loc.at[2 * cc + i], out_hbm.at[pl.ds(i * B, B), :], x_loc.at[i]).start()

    for i in range(2):
        x_to_mate(i).wait_send()
        y_to_mate(2 * (1 - cc) + i).wait_send()
    for it in range(4):
        hp = hp_at(it)
        for m in range(3):
            w_to(m, hp, mate, 0).wait_send()
            if it % 2 == 0:
                for n in range(2):
                    w_on(m, hp, n).wait_send()

    for i in (2, 3):
        x_to_far(i).wait_send()

    def last(i):
        half_to_mate(i).wait_send()
        y_to_far(i).wait_send()

    loop(4, last)
    for i in range(2):
        pltpu.make_async_copy(a_loc.at[2 * cc + i], out_hbm.at[pl.ds(i * B, B), :], x_loc.at[i]).wait()


def solution(mesh):
    bf, f = jnp.bfloat16, jnp.float32
    dma = pltpu.SemaphoreType.DMA

    def step(x, gain, wq, wk, wv, wo):
        hbm = pl.BlockSpec(memory_space=pl.ANY)
        vmem = pl.BlockSpec(memory_space=pltpu.VMEM)
        return pl.pallas_call(
            _kernel,
            out_shape=jax.ShapeDtypeStruct(x.shape, bf),
            in_specs=[hbm, vmem, vmem, hbm, hbm, hbm, hbm],
            out_specs=hbm,
            scratch_shapes=[
                pltpu.VMEM((8, B, 1024), bf),
                pltpu.VMEM((4, B, 1024), bf),
                pltpu.VMEM((3, 4, 1024, 256), bf),
                pltpu.VMEM((1024, 1024), bf),
                pltpu.VMEM((8, 8, B, HEAD), bf),
                pltpu.VMEM((8, 8, HEAD + 16, B), bf),
                pltpu.VMEM((5, 8, B, HEAD), bf),
                pltpu.VMEM((B, 1024), bf),
                pltpu.VMEM((B, HEAD), f),
                pltpu.VMEM((B, HEAD), f),
                pltpu.VMEM((3, QUAD, B), f),
                pltpu.VMEM((3, QUAD, HEAD + 16, B), f),
                pltpu.VMEM((QUAD, B, B), f),
                pltpu.VMEM((QUAD, B), f),
                pltpu.VMEM((2, B, 1024), f),
                pltpu.VMEM((2, B, 1024), bf),
                pltpu.VMEM((2, 2, B // 2, 1024), bf),
                pltpu.VMEM((4, B // 2, 1024), bf),
                dma((3, 4, 3)), dma((3, 4, 4)), dma((3, 2, 2)),
                dma((2,)), dma((2,)), dma((2,)), dma((4,)), dma((4,)), dma((4,)), dma((4,)),
                dma((2,)), dma((2,)), dma((4,)), dma((4,)), dma((4,)), dma((2, 2)), dma((2,)),
            ],
            compiler_params=pltpu.CompilerParams(collective_id=0, has_side_effects=True, vmem_limit_bytes=67043328),
            name="layer",
        )(x, gain, _angles(), wq, wk, wv, wo)

    tokens, whole = P(("dp", "sp"), None), P("sp", None)
    return jax.shard_map(
        step,
        mesh=mesh,
        in_specs=(tokens, P(None), whole, whole, whole, whole),
        out_specs=tokens,
        check_vma=False,
    )
```

```python
import functools

import jax
import jax.numpy as jnp
import numpy as np
from jax import lax
from jax.experimental import pallas as pl
from jax.experimental.pallas import tpu as pltpu
from jax.sharding import PartitionSpec as P

HEAD = 128
THETA = 10000
NEG = -1e30
HIDDEN = 2 * NEG
LOG2E = 1.4426950408889634
B = 512
QUAD = 4
MESH = pl.DeviceIdType.MESH


def _dot(a, b, ca, cb):
    return lax.dot_general(a, b, (((ca,), (cb,)), ((), ())), preferred_element_type=jnp.float32)


def _angles():
    freq = np.float64(THETA) ** (-np.arange(64) / 64)
    freq = np.concatenate([freq, freq])
    sign = np.concatenate([-np.ones(64), np.ones(64)])
    coarse = 64 * np.arange(64)[:, None] * freq
    fine = np.arange(64)[:, None] * freq
    out = np.stack([np.cos(coarse), np.sin(coarse) * sign, np.cos(fine), np.sin(fine) * sign])
    return jnp.asarray(out.astype(np.float32))


def _kernel(x_hbm, gain_ref, ang_ref, wq_hbm, wk_hbm, wv_hbm, wo_hbm, out_hbm,
            xs, a_loc, w, wo, k_s, vt_s, q_s, top_s, mix_s, s_s, peak_s, y_own, from_mate, from_far, half_in,
            w_send, w_recv, w_fwd, x_loc, x_mate_send, x_mate, x_send, x_dir, x_fwd_send, x_fwd,
            mate_send, mate_recv, half_send, half_recv, far_send, far_recv, misc):
    me = lax.axis_index("sp")
    y = lax.axis_index("dp")
    xx, cc = lax.div(me, 2), lax.rem(me, 2)
    mate = 2 * xx + 1 - cc
    far = 2 * (1 - xx) + cc
    far0 = 2 * (1 - xx)
    weights = (wk_hbm, wv_hbm, wq_hbm)
    rows = B // 2
    depth = 256

    barrier = pltpu.get_barrier_semaphore()
    for peer in (mate, far, 2 * (1 - xx) + 1 - cc):
        pl.semaphore_signal(barrier, inc=1, device_id={"dp": y, "sp": peer}, device_id_type=MESH)
    pl.semaphore_signal(barrier, inc=1, device_id={"dp": 1 - y, "sp": me}, device_id_type=MESH)
    pl.semaphore_wait(barrier, 4)

    def remote(src, dst, send, recv, sp, dp=y):
        return pltpu.make_async_remote_copy(src_ref=src, dst_ref=dst, send_sem=send, recv_sem=recv, device_id={"dp": dp, "sp": sp},
                                            device_id_type=MESH)

    def w_place(m, hp, sender):
        return w.at[m, hp, pl.ds(pl.multiple_of(sender * depth, depth), depth), :]

    def w_columns(m, hp, owner):
        return weights[m].at[:, pl.ds(pl.multiple_of(owner * 1024 + hp * 256, 256), 256)]

    def w_to(m, hp, owner, n):
        return remote(w_columns(m, hp, owner), w_place(m, hp, me), w_send.at[m, hp, n], w_recv.at[m, hp, me], owner)

    def w_from(m, hp, sender):
        return remote(w_place(m, hp, sender), w_place(m, hp, sender), misc.at[0], w_recv.at[m, hp, sender], sender)

    def w_on(m, hp, n):
        place = w_place(m, hp, far0 + n)
        return remote(place, place, w_fwd.at[m, lax.div(hp, 2), n], w_recv.at[m, hp, far0 + n], me, 1 - y)

    def w_own(m, hp):
        return pltpu.make_async_copy(w_columns(m, hp, me), w_place(m, hp, me), w_recv.at[m, hp, me])

    def x_own(i):
        return pltpu.make_async_copy(x_hbm.at[pl.ds(i * B, B), :], xs.at[2 * me + i], x_loc.at[i])

    def x_to_mate(i):
        return remote(x_hbm.at[pl.ds(i * B, B), :], xs.at[2 * me + i], x_mate_send.at[i], x_mate.at[i], mate)

    def x_from_mate(i):
        return remote(xs.at[2 * mate + i], xs.at[2 * mate + i], misc.at[0], x_mate.at[i], mate)

    def x_half(b, c):
        return xs.at[b, pl.ds(pl.multiple_of(c * rows, rows), rows), :]

    def x_to_far(i):
        return remote(x_half(4 * xx + i, cc), x_half(4 * xx + i, cc), x_send.at[i], x_dir.at[i], far)

    def x_from_far(i):
        place = x_half(4 * (1 - xx) + i, cc)
        return remote(place, place, misc.at[0], x_dir.at[i], far)

    def x_on(i):
        place = x_half(4 * (1 - xx) + i, cc)
        return remote(place, place, x_fwd_send.at[i], x_fwd.at[i], mate)

    def x_on_from(i):
        place = x_half(4 * (1 - xx) + i, 1 - cc)
        return remote(place, place, misc.at[0], x_fwd.at[i], mate)

    def y_to_mate(i):
        return remote(a_loc.at[i], from_mate.at[lax.rem(i, 2)], mate_send.at[lax.rem(i, 2)], mate_recv.at[lax.rem(i, 2)], mate)

    def y_from_mate(i):
        return remote(from_mate.at[i], from_mate.at[i], misc.at[0], mate_recv.at[i], mate)

    def half_to_mate(i):
        return remote(x_half(4 * (1 - xx) + i, 1 - cc), half_in.at[i], half_send.at[i], half_recv.at[i], mate)

    def half_from_mate(i):
        return remote(half_in.at[i], half_in.at[i], misc.at[0], half_recv.at[i], mate)

    def y_to_far(i):
        owner = 2 * (1 - xx) + lax.div(i, 2)
        return remote(x_half(4 * (1 - xx) + i, cc), from_far.at[lax.rem(i, 2), cc], far_send.at[i], far_recv.at[lax.rem(i, 2), cc], owner)

    def y_from_far(i, c):
        return remote(from_far.at[i, c], from_far.at[i, c], misc.at[0], far_recv.at[i, c], far0 + c)

    def loop(n, body):
        lax.fori_loop(0, n, lambda i, _: (body(i), None)[1], None)

    def hp_at(it):
        return 2 * lax.div(it, 2) + jnp.where(lax.rem(it, 2) == 0, y, 1 - y)

    def crossing(g):
        if isinstance(g, int) and g < 6:
            return [w_to(g % 3, hp_at(2 * (g // 3)), far0 + (cc if n == 1 else 1 - cc), n) for n in (1, 2)]
        return [x_to_far(g - 6)]

    def cross(g):
        for copy in crossing(g - 2):
            copy.wait_send()
        for copy in crossing(g):
            copy.start()

    for g in range(2):
        for copy in crossing(g):
            copy.start()
    for i in range(2):
        x_own(i).start()
        x_to_mate(i).start()
    for it in range(4):
        hp = hp_at(it)
        for m in range(3):
            w_own(m, hp).start()
            w_to(m, hp, mate, 0).start()
    wo_copy = pltpu.make_async_copy(wo_hbm, wo, misc.at[1])
    wo_copy.start()

    def arrive(m, hp, onward):
        for n in range(2):
            w_from(m, hp, far0 + n).wait_recv()
            if onward:
                w_on(m, hp, n).start()

    arrive(0, hp_at(0), True)
    cross(2)
    for i in range(2):
        x_own(i).wait()
    for i in range(2):
        x_from_mate(i).wait_recv()

    gain = gain_ref[...].astype(jnp.float32)[None, :]

    def norm_rows(src, dst, here):
        wide = src[here, :].astype(jnp.float32)
        scale = lax.rsqrt(jnp.mean(wide * wide, -1, keepdims=True) + 1e-6)
        dst[here, :] = (wide * scale * gain).astype(jnp.bfloat16)

    def norm(src, dst):
        loop(B // 256, lambda r: norm_rows(src, dst, pl.ds(pl.multiple_of(r * 256, 256), 256)))

    def turn_table(b):
        cos, sin = [], []
        for r in range(B // 64):
            at = pl.ds(b * (B // 64) + r, 1)
            ch, sh, cf, sf = ang_ref[0, at, :], ang_ref[1, at, :], ang_ref[2], ang_ref[3]
            cos.append(ch * cf - sh * sf)
            sin.append(sh * cf + ch * sf)
        return jnp.concatenate(cos, axis=0), jnp.concatenate(sin, axis=0)

    def turned(t, table):
        t = t.astype(jnp.float32)
        return (t * table[0] + pltpu.roll(t, 64, 1) * table[1]).astype(jnp.bfloat16)

    def project(a, m, hp, b, slot, table):
        t = _dot(a[...], w[m, hp], 1, 0).astype(jnp.bfloat16)
        for i in range(2):
            part = t[:, i * HEAD : (i + 1) * HEAD]
            if m == 0:
                k_s[b, 2 * hp + i] = turned(part, table)
            elif m == 1:
                vt_s[b, 2 * hp + i, 0:HEAD, :] = part.T
            else:
                q_s[slot, 2 * hp + i] = turned(part, table)

    e = HEAD**-0.5 * LOG2E

    def scores(j, slot, h, n):
        s = _dot(k_s[j, h], q_s[slot, h], 1, 1)
        peak_s[n : n + 1, :] = s.max(axis=0, keepdims=True)
        s_s[n] = s

    def attend(qb, slot, quad, lo, hi, after, *, diagonal=True, state=0, first=True, final=True, between=None):
        @pl.when(first)
        def _():
            for n in range(QUAD):
                scores(lo, slot, quad * QUAD + n, n)

        def whole(j):
            more = diagonal | (j + 1 < hi)
            key, where, which = jnp.where(more, j + 1, after[0]), jnp.where(more, slot, after[1]), jnp.where(more, quad, after[2])
            for n in range(QUAD):
                old = top_s[state, n : n + 1, :]
                top = jnp.maximum(old, peak_s[n : n + 1, :])
                top_s[state, n : n + 1, :] = top
                p = jnp.exp2((s_s[n] - top) * e).astype(jnp.bfloat16)
                scores(key, where, which * QUAD + n, n)
                mix_s[state, n] = mix_s[state, n] * jnp.exp2((old - top) * e) + _dot(vt_s[j, quad * QUAD + n], p, 1, 0)

        def finish():
            for n in range(QUAD):
                out = mix_s[state, n, 0:HEAD, :] * (1 / mix_s[state, n, HEAD : HEAD + 1, :])
                q_s[slot, quad * QUAD + n] = out.T.astype(jnp.bfloat16)
                mix_s[state, n] = jnp.zeros(mix_s.shape[2:], jnp.float32)
            top_s[state] = jnp.full(top_s.shape[1:], NEG, jnp.float32)

        def two(t):
            whole(lo + 2 * t)
            whole(lo + 2 * t + 1)

        loop(lax.div(hi - lo, 2), two)

        @pl.when(lax.rem(hi - lo, 2) == 1)
        def _():
            whole(hi - 1)

        if between is not None:
            between()

        @pl.when(diagonal)
        def _():
            half = B // 2
            ok = lax.broadcasted_iota(jnp.int32, (half, half), 1) >= lax.broadcasted_iota(jnp.int32, (half, half), 0)
            for n in range(QUAD):
                h = quad * QUAD + n
                for at in (0, half):
                    cols = slice(at, at + half)
                    parts = [s_s[n, 0:half, cols], jnp.where(ok, s_s[n, half:B, cols], HIDDEN)] if at else [jnp.where(ok, s_s[n, 0:half, cols], HIDDEN)]
                    old = top_s[state, n : n + 1, cols]
                    top = old
                    for part in parts:
                        top = jnp.maximum(top, part.max(axis=0, keepdims=True))
                    top_s[state, n : n + 1, cols] = top
                    p = jnp.concatenate([jnp.exp2((part - top) * e).astype(jnp.bfloat16) for part in parts], axis=0)
                    mix_s[state, n, :, cols] = (mix_s[state, n, :, cols] * jnp.exp2((old - top) * e)
                                                + _dot(vt_s[qb, h, :, 0 : at + half], p, 1, 0))
                scores(after[0], after[1], after[2] * QUAD + n, n)
            if final is True:
                finish()

        if final is not True:
            pl.when(final)(finish)
        elif diagonal is not True:
            pl.when(jnp.logical_not(diagonal))(finish)

    def combine(i):
        def part(r):
            here = pl.ds(pl.multiple_of(cc * rows + r * 64, 64), 64)
            at = pl.ds(pl.multiple_of(r * 64, 64), 64)
            b = 4 * (1 - xx) + i
            xs[b, here, :] = (xs[b, here, :].astype(jnp.float32) + half_in[i, at, :].astype(jnp.float32)).astype(jnp.bfloat16)

        loop(rows // 64, part)

    top_s[...] = jnp.full(top_s.shape, NEG, jnp.float32)
    mix_s[...] = jnp.zeros(mix_s.shape, jnp.float32)
    vt_s[:, :, HEAD:, :] = jnp.ones(vt_s.shape[:2] + (vt_s.shape[2] - HEAD, B), jnp.bfloat16)
    loop(4, lambda i: norm(xs.at[4 * xx + i], a_loc.at[i]))

    def pair(it):
        hp = hp_at(it)

        def when(n, work):
            @pl.when(it == n)
            def _():
                for m, at, onward, then in work:
                    arrive(m, hp_at(at), onward)
                    if then is not None:
                        cross(then)

        for m in range(3):
            w_own(m, hp).wait()
            w_from(m, hp, mate).wait_recv()
            when(0, [[], [(1, 0, True, 3)], [(2, 0, True, 4)]][m])
            when(1, [[(0, 1, False, None)], [(1, 1, False, None)], [(0, 2, True, 5), (2, 1, False, None)]][m])
            when(2, [[], [], [(2, 2, True, 7)]][m])
            when(3, [(m, 3, False, None)])
            for i in range(4):
                b = 4 * xx + i
                project(a_loc.at[i], m, hp, b, i, None if m == 1 else turn_table(b))

        @pl.when((it == 1) | (it == 2) | ((it == 3) & (xx == 1)))
        def _():
            blk = jnp.where(it == 2, 2, 3)
            short = it == 3
            quad = jnp.where(short, 1, 0)
            attend(4 * xx + blk, blk, quad, 4 * xx, 4 * xx + blk - quad, (jnp.where(short, 6, 0), 3, quad), diagonal=jnp.logical_not(short),
                   state=xx * jnp.where(it == 1, 1, jnp.where(short, 2, 3)), final=xx == 0, between=lambda: when(1, [(1, 2, True, 6)]))

    loop(4, pair)
    wo_copy.wait()

    first = 1 - xx

    def forward_x(i):
        x_from_far(i).wait_recv()
        x_on(i).start()

    def x_here(i):
        x_on(i).wait_send()
        x_on_from(i).wait_recv()

    a_far = a_loc.at[2 * cc]

    @pl.when(xx == 1)
    def _():
        forward_x(0)
        attend(7, 3, 1, 6, 7, (0, 4, 0), state=2, first=False, final=False)

    def blocks(s):
        i = s - first
        away = (i >= 0) & (i < 4)
        qb = jnp.where(xx == 1, s, jnp.where(s < 1, s, jnp.where(s < 5, s + 3, s - 4)))
        here = qb - 4 * xx
        return i, away, qb, here, jnp.where(away, 4, here)

    def step(s):
        @pl.when((s == 1) | (s == 2))
        def _():
            cross(s + 7)

        i, away, qb, here, slot = blocks(s)
        next_slot = blocks(s + 1)[-1]

        @pl.when(i == 0)
        def _():
            x_here(0)
            norm(xs.at[qb], a_far)

        @pl.when(away)
        def _():
            table = turn_table(qb)
            for hp in range(4):
                for m in range(3):
                    project(a_far, m, hp, qb, 4, table)

        def quad(n):
            resume = (xx == 1) & ((s == 7) | ((s == 6) & (n == 0)))

            @pl.when(jnp.logical_not((xx == 0) & (s >= 6) & (n == 0)))
            def _():
                attend(qb, slot, n, 0, jnp.where(resume, 4, qb),
                       (0, jnp.where(n == 0, slot, next_slot), jnp.where((n == 0) | ((s >= 5) & (xx == 0)), 1, 0)),
                       diagonal=jnp.logical_not(resume), state=jnp.where(resume, jnp.where(s == 7, 1 + n, 3), 0),
                       first=(n == 0) & (away | (s == 0)))

            @pl.when((n == 0) & (i >= -1) & (i < 3))
            def _():
                forward_x(i + 1)

            @pl.when((n == 0) & (i >= 1) & (i < 5))
            def _():
                half_from_mate(i - 1).wait_recv()
                combine(i - 1)
                y_to_far(i - 1).start()

        loop(8 // QUAD, quad)

        own = jnp.logical_not(away) & (lax.div(here, 2) == cc)

        def output(store):
            seen = jnp.concatenate([q_s[slot, h] for h in range(8)], axis=1)
            for n in range(4):
                cols = slice(n * 256, n * 256 + 256)
                store(cols, _dot(seen, wo[:, cols], 1, 0))

        @pl.when(own)
        def _():
            def store(cols, r):
                y_own[lax.rem(here, 2), :, cols] = r

            output(store)

        @pl.when(away & (i < 3))
        def _():
            x_here(i + 1)

        @pl.when(away)
        def _():
            after = 4 * (1 - xx) + jnp.minimum(i + 1, 3)
            for r in range(B // 64):
                norm_rows(xs.at[after], a_far, slice(r * 64, r * 64 + 64))

            def store(cols, r):
                xs[qb, :, cols] = r.astype(jnp.bfloat16)

            output(store)

        @pl.when(jnp.logical_not(own | away))
        def _():
            def store(cols, r):
                a_loc[here, :, cols] = r.astype(jnp.bfloat16)

            output(store)

        @pl.when(away)
        def _():
            half_to_mate(i).start()

        @pl.when(jnp.logical_not(own | away))
        def _():
            y_to_mate(here).start()

    loop(8, step)

    for i in range(2):
        y_from_mate(i).wait_recv()
        for c in range(2):
            y_from_far(i, c).wait_recv()
            base = c * rows

            def part(r):
                here = pl.ds(pl.multiple_of(base + r * 128, 128), 128)
                at = pl.ds(pl.multiple_of(r * 128, 128), 128)
                f = jnp.float32
                total = y_own[i, here, :] + from_mate[i, here, :].astype(f) + from_far[i, c, at, :].astype(f)
                a_loc[2 * cc + i, here, :] = (xs[2 * me + i, here, :].astype(f) + total).astype(jnp.bfloat16)

            loop(rows // 128, part)
        pltpu.make_async_copy(a_loc.at[2 * cc + i], out_hbm.at[pl.ds(i * B, B), :], x_loc.at[i]).start()

    for i in range(2):
        x_to_mate(i).wait_send()
        y_to_mate(2 * (1 - cc) + i).wait_send()
    for it in range(4):
        hp = hp_at(it)
        for m in range(3):
            w_to(m, hp, mate, 0).wait_send()
            if it % 2 == 0:
                for n in range(2):
                    w_on(m, hp, n).wait_send()

    for i in (2, 3):
        x_to_far(i).wait_send()

    def last(i):
        half_to_mate(i).wait_send()
        y_to_far(i).wait_send()

    loop(4, last)
    for i in range(2):
        pltpu.make_async_copy(a_loc.at[2 * cc + i], out_hbm.at[pl.ds(i * B, B), :], x_loc.at[i]).wait()


def solution(mesh):
    bf, f = jnp.bfloat16, jnp.float32
    dma = pltpu.SemaphoreType.DMA

    def step(x, gain, wq, wk, wv, wo):
        hbm = pl.BlockSpec(memory_space=pl.ANY)
        vmem = pl.BlockSpec(memory_space=pltpu.VMEM)
        return pl.pallas_call(
            _kernel,
            out_shape=jax.ShapeDtypeStruct(x.shape, bf),
            in_specs=[hbm, vmem, vmem, hbm, hbm, hbm, hbm],
            out_specs=hbm,
            scratch_shapes=[
                pltpu.VMEM((8, B, 1024), bf),
                pltpu.VMEM((4, B, 1024), bf),
                pltpu.VMEM((3, 4, 1024, 256), bf),
                pltpu.VMEM((1024, 1024), bf),
                pltpu.VMEM((8, 8, B, HEAD), bf),
                pltpu.VMEM((8, 8, HEAD + 16, B), bf),
                pltpu.VMEM((5, 8, B, HEAD), bf),
                pltpu.VMEM((4, QUAD, B), f),
                pltpu.VMEM((4, QUAD, HEAD + 16, B), f),
                pltpu.VMEM((QUAD, B, B), f),
                pltpu.VMEM((QUAD, B), f),
                pltpu.VMEM((2, B, 1024), f),
                pltpu.VMEM((2, B, 1024), bf),
                pltpu.VMEM((2, 2, B // 2, 1024), bf),
                pltpu.VMEM((4, B // 2, 1024), bf),
                dma((3, 4, 3)), dma((3, 4, 4)), dma((3, 2, 2)),
                dma((2,)), dma((2,)), dma((2,)), dma((4,)), dma((4,)), dma((4,)), dma((4,)),
                dma((2,)), dma((2,)), dma((4,)), dma((4,)), dma((4,)), dma((2, 2)), dma((2,)),
            ],
            compiler_params=pltpu.CompilerParams(collective_id=0, has_side_effects=True, vmem_limit_bytes=67043328),
            name="layer",
        )(x, gain, _angles(), wq, wk, wv, wo)

    tokens, whole = P(("dp", "sp"), None), P("sp", None)
    return jax.shard_map(
        step,
        mesh=mesh,
        in_specs=(tokens, P(None), whole, whole, whole, whole),
        out_specs=tokens,
        check_vma=False,
    )
```

```python
import functools

import jax
import jax.numpy as jnp
import numpy as np
from jax import lax
from jax.experimental import pallas as pl
from jax.experimental.pallas import tpu as pltpu
from jax.sharding import PartitionSpec as P

HEAD = 128
THETA = 10000
NEG = -1e30
HIDDEN = 2 * NEG
LOG2E = 1.4426950408889634
B = 512
QUAD = 4
MESH = pl.DeviceIdType.MESH


def _dot(a, b, ca, cb):
    return lax.dot_general(a, b, (((ca,), (cb,)), ((), ())), preferred_element_type=jnp.float32)


def _angles():
    freq = np.float64(THETA) ** (-np.arange(64) / 64)
    freq = np.concatenate([freq, freq])
    sign = np.concatenate([-np.ones(64), np.ones(64)])
    coarse = 64 * np.arange(64)[:, None] * freq
    fine = np.arange(64)[:, None] * freq
    out = np.stack([np.cos(coarse), np.sin(coarse) * sign, np.cos(fine), np.sin(fine) * sign])
    return jnp.asarray(out.astype(np.float32))


def _kernel(x_hbm, gain_ref, ang_ref, wq_hbm, wk_hbm, wv_hbm, wo_hbm, out_hbm,
            xs, a_loc, w, wo, k_s, vt_s, q_s, top_s, mix_s, s_s, peak_s, y_own, from_mate, from_far, half_in,
            w_send, w_recv, w_fwd, x_loc, x_mate_send, x_mate, x_send, x_dir, x_fwd_send, x_fwd,
            mate_send, mate_recv, half_send, half_recv, far_send, far_recv, misc):
    me = lax.axis_index("sp")
    y = lax.axis_index("dp")
    xx, cc = lax.div(me, 2), lax.rem(me, 2)
    mate = 2 * xx + 1 - cc
    far = 2 * (1 - xx) + cc
    far0 = 2 * (1 - xx)
    weights = (wk_hbm, wv_hbm, wq_hbm)
    rows = B // 2
    depth = 256

    barrier = pltpu.get_barrier_semaphore()
    for peer in (mate, far, 2 * (1 - xx) + 1 - cc):
        pl.semaphore_signal(barrier, inc=1, device_id={"dp": y, "sp": peer}, device_id_type=MESH)
    pl.semaphore_signal(barrier, inc=1, device_id={"dp": 1 - y, "sp": me}, device_id_type=MESH)
    pl.semaphore_wait(barrier, 4)

    def remote(src, dst, send, recv, sp, dp=y):
        return pltpu.make_async_remote_copy(src_ref=src, dst_ref=dst, send_sem=send, recv_sem=recv, device_id={"dp": dp, "sp": sp},
                                            device_id_type=MESH)

    def w_place(m, hp, sender):
        return w.at[m, hp, pl.ds(pl.multiple_of(sender * depth, depth), depth), :]

    def w_columns(m, hp, owner):
        return weights[m].at[:, pl.ds(pl.multiple_of(owner * 1024 + hp * 256, 256), 256)]

    def w_to(m, hp, owner, n):
        return remote(w_columns(m, hp, owner), w_place(m, hp, me), w_send.at[m, hp, n], w_recv.at[m, hp, me], owner)

    def w_from(m, hp, sender):
        return remote(w_place(m, hp, sender), w_place(m, hp, sender), misc.at[0], w_recv.at[m, hp, sender], sender)

    def w_on(m, hp, n):
        place = w_place(m, hp, far0 + n)
        return remote(place, place, w_fwd.at[m, lax.div(hp, 2), n], w_recv.at[m, hp, far0 + n], me, 1 - y)

    def w_own(m, hp):
        return pltpu.make_async_copy(w_columns(m, hp, me), w_place(m, hp, me), w_recv.at[m, hp, me])

    def x_own(i):
        return pltpu.make_async_copy(x_hbm.at[pl.ds(i * B, B), :], xs.at[2 * me + i], x_loc.at[i])

    def x_to_mate(i):
        return remote(x_hbm.at[pl.ds(i * B, B), :], xs.at[2 * me + i], x_mate_send.at[i], x_mate.at[i], mate)

    def x_from_mate(i):
        return remote(xs.at[2 * mate + i], xs.at[2 * mate + i], misc.at[0], x_mate.at[i], mate)

    def x_half(b, c):
        return xs.at[b, pl.ds(pl.multiple_of(c * rows, rows), rows), :]

    def x_to_far(i):
        return remote(x_half(4 * xx + i, cc), x_half(4 * xx + i, cc), x_send.at[i], x_dir.at[i], far)

    def x_from_far(i):
        place = x_half(4 * (1 - xx) + i, cc)
        return remote(place, place, misc.at[0], x_dir.at[i], far)

    def x_on(i):
        place = x_half(4 * (1 - xx) + i, cc)
        return remote(place, place, x_fwd_send.at[i], x_fwd.at[i], mate)

    def x_on_from(i):
        place = x_half(4 * (1 - xx) + i, 1 - cc)
        return remote(place, place, misc.at[0], x_fwd.at[i], mate)

    def y_to_mate(i):
        return remote(a_loc.at[i], from_mate.at[lax.rem(i, 2)], mate_send.at[lax.rem(i, 2)], mate_recv.at[lax.rem(i, 2)], mate)

    def y_from_mate(i):
        return remote(from_mate.at[i], from_mate.at[i], misc.at[0], mate_recv.at[i], mate)

    def half_to_mate(i):
        return remote(x_half(4 * (1 - xx) + i, 1 - cc), half_in.at[i], half_send.at[i], half_recv.at[i], mate)

    def half_from_mate(i):
        return remote(half_in.at[i], half_in.at[i], misc.at[0], half_recv.at[i], mate)

    def y_to_far(i):
        owner = 2 * (1 - xx) + lax.div(i, 2)
        return remote(x_half(4 * (1 - xx) + i, cc), from_far.at[lax.rem(i, 2), cc], far_send.at[i], far_recv.at[lax.rem(i, 2), cc], owner)

    def y_from_far(i, c):
        return remote(from_far.at[i, c], from_far.at[i, c], misc.at[0], far_recv.at[i, c], far0 + c)

    def loop(n, body):
        lax.fori_loop(0, n, lambda i, _: (body(i), None)[1], None)

    def hp_at(it):
        return 2 * lax.div(it, 2) + jnp.where(lax.rem(it, 2) == 0, y, 1 - y)

    def crossing(g):
        if isinstance(g, int) and g < 6:
            return [w_to(g % 3, hp_at(2 * (g // 3)), far0 + (cc if n == 1 else 1 - cc), n) for n in (1, 2)]
        return [x_to_far(g - 6)]

    def cross(g):
        for copy in crossing(g - 2):
            copy.wait_send()
        for copy in crossing(g):
            copy.start()

    for g in range(2):
        for copy in crossing(g):
            copy.start()
    for i in range(2):
        x_own(i).start()
        x_to_mate(i).start()
    for it in range(4):
        hp = hp_at(it)
        for m in range(3):
            w_own(m, hp).start()
            w_to(m, hp, mate, 0).start()
    wo_copy = pltpu.make_async_copy(wo_hbm, wo, misc.at[1])
    wo_copy.start()

    def arrive(m, hp, onward):
        for n in range(2):
            w_from(m, hp, far0 + n).wait_recv()
            if onward:
                w_on(m, hp, n).start()

    arrive(0, hp_at(0), True)
    cross(2)
    for i in range(2):
        x_own(i).wait()
    for i in range(2):
        x_from_mate(i).wait_recv()

    gain = gain_ref[...].astype(jnp.float32)[None, :]

    def norm_rows(src, dst, here):
        wide = src[here, :].astype(jnp.float32)
        scale = lax.rsqrt(jnp.mean(wide * wide, -1, keepdims=True) + 1e-6)
        dst[here, :] = (wide * scale * gain).astype(jnp.bfloat16)

    def norm(src, dst):
        loop(B // 256, lambda r: norm_rows(src, dst, pl.ds(pl.multiple_of(r * 256, 256), 256)))

    def turn_table(b):
        cos, sin = [], []
        for r in range(B // 64):
            at = pl.ds(b * (B // 64) + r, 1)
            ch, sh, cf, sf = ang_ref[0, at, :], ang_ref[1, at, :], ang_ref[2], ang_ref[3]
            cos.append(ch * cf - sh * sf)
            sin.append(sh * cf + ch * sf)
        return jnp.concatenate(cos, axis=0), jnp.concatenate(sin, axis=0)

    def turned(t, table):
        t = t.astype(jnp.float32)
        return (t * table[0] + pltpu.roll(t, 64, 1) * table[1]).astype(jnp.bfloat16)

    def project(a, m, hp, b, slot, table):
        t = _dot(a[...], w[m, hp], 1, 0).astype(jnp.bfloat16)
        for i in range(2):
            part = t[:, i * HEAD : (i + 1) * HEAD]
            if m == 0:
                k_s[b, 2 * hp + i] = turned(part, table)
            elif m == 1:
                vt_s[b, 2 * hp + i] = part.T
            else:
                q_s[slot, 2 * hp + i] = turned(part, table)

    e = HEAD**-0.5 * LOG2E

    half = B // 2
    halves = [(n, slice(at, at + half)) for n in range(QUAD) for at in (0, half)]

    def scores(j, slot, quad, n, cols):
        s = _dot(k_s[j, quad * QUAD + n], q_s[slot, quad * QUAD + n, cols, :], 1, 1)
        peak_s[n : n + 1, cols] = s.max(axis=0, keepdims=True)
        s_s[n, :, cols] = s

    def values(j, h, keys):
        return jnp.concatenate([vt_s[j, h, :, 0:keys], jnp.ones((16, keys), jnp.bfloat16)], axis=0)

    def attend(qb, slot, quad, lo, hi, after, *, diagonal=True, state=0, first=True, final=True, between=None, sizes=(2, 1)):
        @pl.when(first)
        def _():
            for n, cols in halves:
                scores(lo, slot, quad, n, cols)

        def whole(j):
            more = diagonal | (j + 1 < hi)
            key, where, which = jnp.where(more, j + 1, after[0]), jnp.where(more, slot, after[1]), jnp.where(more, quad, after[2])
            for n, cols in halves:
                old = top_s[state, n : n + 1, cols]
                top = jnp.maximum(old, peak_s[n : n + 1, cols])
                top_s[state, n : n + 1, cols] = top
                p = jnp.exp2((s_s[n, :, cols] - top) * e).astype(jnp.bfloat16)
                scores(key, where, which, n, cols)
                mix_s[state, n, :, cols] = mix_s[state, n, :, cols] * jnp.exp2((old - top) * e) + _dot(values(j, quad * QUAD + n, B), p, 1, 0)

        def finish():
            for n in range(QUAD):
                out = mix_s[state, n, 0:HEAD, :] * (1 / mix_s[state, n, HEAD : HEAD + 1, :])
                q_s[slot, quad * QUAD + n] = out.T.astype(jnp.bfloat16)
                mix_s[state, n] = jnp.zeros(mix_s.shape[2:], jnp.float32)
            top_s[state] = jnp.full(top_s.shape[1:], NEG, jnp.float32)

        count, at = hi - lo, lo
        for size in sizes:
            turns = lax.div(count, size)
            turn = lambda t, size=size, at=at: [whole(at + size * t + n) for n in range(size)] and None
            if size == sizes[0] and len(sizes) > 1:
                loop(turns, turn)
            else:
                pl.when(turns == 1)(functools.partial(turn, 0))
            at, count = at + size * turns, count - size * turns

        if between is not None:
            between()

        @pl.when(diagonal)
        def _():
            ok = lax.broadcasted_iota(jnp.int32, (half, half), 1) >= lax.broadcasted_iota(jnp.int32, (half, half), 0)
            for n in range(QUAD):
                h = quad * QUAD + n
                for at in (0, half):
                    cols = slice(at, at + half)
                    parts = [s_s[n, 0:half, cols], jnp.where(ok, s_s[n, half:B, cols], HIDDEN)] if at else [jnp.where(ok, s_s[n, 0:half, cols], HIDDEN)]
                    old = top_s[state, n : n + 1, cols]
                    top = old
                    for part in parts:
                        top = jnp.maximum(top, part.max(axis=0, keepdims=True))
                    top_s[state, n : n + 1, cols] = top
                    p = jnp.concatenate([jnp.exp2((part - top) * e).astype(jnp.bfloat16) for part in parts], axis=0)
                    mix_s[state, n, :, cols] = mix_s[state, n, :, cols] * jnp.exp2((old - top) * e) + _dot(values(qb, h, at + half), p, 1, 0)
                    if at:
                        for c in (slice(0, half), slice(half, B)):
                            scores(after[0], after[1], after[2], n, c)
            if final is True:
                finish()

        if final is not True:
            pl.when(final)(finish)
        elif diagonal is not True:
            pl.when(jnp.logical_not(diagonal))(finish)

    def combine(i):
        def part(r):
            here = pl.ds(pl.multiple_of(cc * rows + r * 64, 64), 64)
            at = pl.ds(pl.multiple_of(r * 64, 64), 64)
            b = 4 * (1 - xx) + i
            xs[b, here, :] = (xs[b, here, :].astype(jnp.float32) + half_in[i, at, :].astype(jnp.float32)).astype(jnp.bfloat16)

        loop(rows // 64, part)

    top_s[...] = jnp.full(top_s.shape, NEG, jnp.float32)
    mix_s[...] = jnp.zeros(mix_s.shape, jnp.float32)
    loop(4, lambda i: norm(xs.at[4 * xx + i], a_loc.at[i]))

    def pair(it):
        hp = hp_at(it)

        def when(n, work):
            @pl.when(it == n)
            def _():
                for m, at, onward, then in work:
                    arrive(m, hp_at(at), onward)
                    if then is not None:
                        cross(then)

        for m in range(3):
            w_own(m, hp).wait()
            w_from(m, hp, mate).wait_recv()
            when(0, [[], [(1, 0, True, 3)], [(2, 0, True, 4)]][m])
            when(1, [[(0, 1, False, None)], [(1, 1, False, None)], [(0, 2, True, 5), (2, 1, False, None)]][m])
            when(2, [[], [], [(2, 2, True, 7)]][m])
            when(3, [(m, 3, False, None)])
            for i in range(4):
                b = 4 * xx + i
                project(a_loc.at[i], m, hp, b, i, None if m == 1 else turn_table(b))

        @pl.when((it == 1) | (it == 2) | ((it == 3) & (xx == 1)))
        def _():
            blk = jnp.where(it == 2, 2, 3)
            short = it == 3
            quad = jnp.where(short, 1, 0)
            attend(4 * xx + blk, blk, quad, 4 * xx, 4 * xx + blk - quad, (jnp.where(short, 6, 0), 3, quad), diagonal=jnp.logical_not(short),
                   state=xx * jnp.where(it == 1, 1, jnp.where(short, 2, 3)), final=xx == 0, between=lambda: when(1, [(1, 2, True, 6)]))

    loop(4, pair)
    wo_copy.wait()

    first = 1 - xx

    def forward_x(i):
        x_from_far(i).wait_recv()
        x_on(i).start()

    def x_here(i):
        x_on(i).wait_send()
        x_on_from(i).wait_recv()

    a_far = a_loc.at[2 * cc]

    @pl.when(xx == 1)
    def _():
        forward_x(0)
        attend(7, 3, 1, 6, 7, (0, 4, 0), state=2, first=False, final=False, sizes=(1,))

    def blocks(s):
        i = s - first
        away = (i >= 0) & (i < 4)
        qb = jnp.where(xx == 1, s, jnp.where(s < 1, s, jnp.where(s < 5, s + 3, s - 4)))
        here = qb - 4 * xx
        return i, away, qb, here, jnp.where(away, 4, here)

    def step(s):
        @pl.when((s == 1) | (s == 2))
        def _():
            cross(s + 7)

        i, away, qb, here, slot = blocks(s)
        next_slot = blocks(s + 1)[-1]

        @pl.when(i == 0)
        def _():
            x_here(0)
            norm(xs.at[qb], a_far)

        @pl.when(away)
        def _():
            table = turn_table(qb)
            for hp in range(4):
                for m in range(3):
                    project(a_far, m, hp, qb, 4, table)

        def quad(n):
            resume = (xx == 1) & ((s == 7) | ((s == 6) & (n == 0)))

            @pl.when(jnp.logical_not((xx == 0) & (s >= 6) & (n == 0)))
            def _():
                attend(qb, slot, n, 0, jnp.where(resume, 4, qb),
                       (0, jnp.where(n == 0, slot, next_slot), jnp.where((n == 0) | ((s >= 5) & (xx == 0)), 1, 0)),
                       diagonal=jnp.logical_not(resume), state=jnp.where(resume, jnp.where(s == 7, 1 + n, 3), 0),
                       first=(n == 0) & (away | (s == 0)), sizes=(4, 2, 1))

            @pl.when((n == 0) & (i >= -1) & (i < 3))
            def _():
                forward_x(i + 1)

            @pl.when((n == 0) & (i >= 1) & (i < 5))
            def _():
                half_from_mate(i - 1).wait_recv()
                combine(i - 1)
                y_to_far(i - 1).start()

        loop(8 // QUAD, quad)

        own = jnp.logical_not(away) & (lax.div(here, 2) == cc)

        def output(store):
            seen = jnp.concatenate([q_s[slot, h] for h in range(8)], axis=1)
            for n in range(4):
                cols = slice(n * 256, n * 256 + 256)
                store(cols, _dot(seen, wo[:, cols], 1, 0))

        @pl.when(own)
        def _():
            def store(cols, r):
                y_own[lax.rem(here, 2), :, cols] = r

            output(store)

        @pl.when(away & (i < 3))
        def _():
            x_here(i + 1)

        @pl.when(away)
        def _():
            after = 4 * (1 - xx) + jnp.minimum(i + 1, 3)
            for r in range(B // 64):
                norm_rows(xs.at[after], a_far, slice(r * 64, r * 64 + 64))

            def store(cols, r):
                xs[qb, :, cols] = r.astype(jnp.bfloat16)

            output(store)

        @pl.when(jnp.logical_not(own | away))
        def _():
            def store(cols, r):
                a_loc[here, :, cols] = r.astype(jnp.bfloat16)

            output(store)

        @pl.when(away)
        def _():
            half_to_mate(i).start()

        @pl.when(jnp.logical_not(own | away))
        def _():
            y_to_mate(here).start()

    loop(8, step)

    for i in range(2):
        y_from_mate(i).wait_recv()
        for c in range(2):
            y_from_far(i, c).wait_recv()
            base = c * rows

            def part(r):
                here = pl.ds(pl.multiple_of(base + r * 128, 128), 128)
                at = pl.ds(pl.multiple_of(r * 128, 128), 128)
                f = jnp.float32
                total = y_own[i, here, :] + from_mate[i, here, :].astype(f) + from_far[i, c, at, :].astype(f)
                a_loc[2 * cc + i, here, :] = (xs[2 * me + i, here, :].astype(f) + total).astype(jnp.bfloat16)

            loop(rows // 128, part)
        pltpu.make_async_copy(a_loc.at[2 * cc + i], out_hbm.at[pl.ds(i * B, B), :], x_loc.at[i]).start()

    for i in range(2):
        x_to_mate(i).wait_send()
        y_to_mate(2 * (1 - cc) + i).wait_send()
    for it in range(4):
        hp = hp_at(it)
        for m in range(3):
            w_to(m, hp, mate, 0).wait_send()
            if it % 2 == 0:
                for n in range(2):
                    w_on(m, hp, n).wait_send()

    for i in (2, 3):
        x_to_far(i).wait_send()

    def last(i):
        half_to_mate(i).wait_send()
        y_to_far(i).wait_send()

    loop(4, last)
    for i in range(2):
        pltpu.make_async_copy(a_loc.at[2 * cc + i], out_hbm.at[pl.ds(i * B, B), :], x_loc.at[i]).wait()


def solution(mesh):
    bf, f = jnp.bfloat16, jnp.float32
    dma = pltpu.SemaphoreType.DMA

    def step(x, gain, wq, wk, wv, wo):
        hbm = pl.BlockSpec(memory_space=pl.ANY)
        vmem = pl.BlockSpec(memory_space=pltpu.VMEM)
        return pl.pallas_call(
            _kernel,
            out_shape=jax.ShapeDtypeStruct(x.shape, bf),
            in_specs=[hbm, vmem, vmem, hbm, hbm, hbm, hbm],
            out_specs=hbm,
            scratch_shapes=[
                pltpu.VMEM((8, B, 1024), bf),
                pltpu.VMEM((4, B, 1024), bf),
                pltpu.VMEM((3, 4, 1024, 256), bf),
                pltpu.VMEM((1024, 1024), bf),
                pltpu.VMEM((8, 8, B, HEAD), bf),
                pltpu.VMEM((8, 8, HEAD, B), bf),
                pltpu.VMEM((5, 8, B, HEAD), bf),
                pltpu.VMEM((4, QUAD, B), f),
                pltpu.VMEM((4, QUAD, HEAD + 16, B), f),
                pltpu.VMEM((QUAD, B, B), f),
                pltpu.VMEM((QUAD, B), f),
                pltpu.VMEM((2, B, 1024), f),
                pltpu.VMEM((2, B, 1024), bf),
                pltpu.VMEM((2, 2, B // 2, 1024), bf),
                pltpu.VMEM((4, B // 2, 1024), bf),
                dma((3, 4, 3)), dma((3, 4, 4)), dma((3, 2, 2)),
                dma((2,)), dma((2,)), dma((2,)), dma((4,)), dma((4,)), dma((4,)), dma((4,)),
                dma((2,)), dma((2,)), dma((4,)), dma((4,)), dma((4,)), dma((2, 2)), dma((2,)),
            ],
            compiler_params=pltpu.CompilerParams(collective_id=0, has_side_effects=True, vmem_limit_bytes=67043328),
            name="layer",
        )(x, gain, _angles(), wq, wk, wv, wo)

    tokens, whole = P(("dp", "sp"), None), P("sp", None)
    return jax.shard_map(
        step,
        mesh=mesh,
        in_specs=(tokens, P(None), whole, whole, whole, whole),
        out_specs=tokens,
        check_vma=False,
    )
```

```python
import functools

import jax
import jax.numpy as jnp
import numpy as np
from jax import lax
from jax.experimental import pallas as pl
from jax.experimental.pallas import tpu as pltpu
from jax.sharding import PartitionSpec as P

HEAD = 128
THETA = 10000
NEG = -1e30
HIDDEN = 2 * NEG
LOG2E = 1.4426950408889634
B = 512
QUAD = 4
MESH = pl.DeviceIdType.MESH


def _dot(a, b, ca, cb):
    return lax.dot_general(a, b, (((ca,), (cb,)), ((), ())), preferred_element_type=jnp.float32)


def _angles():
    freq = np.float64(THETA) ** (-np.arange(64) / 64)
    freq = np.concatenate([freq, freq])
    sign = np.concatenate([-np.ones(64), np.ones(64)])
    coarse = 64 * np.arange(64)[:, None] * freq
    fine = np.arange(64)[:, None] * freq
    out = np.stack([np.cos(coarse), np.sin(coarse) * sign, np.cos(fine), np.sin(fine) * sign])
    return jnp.asarray(out.astype(np.float32))


def _kernel(x_hbm, gain_ref, ang_ref, wq_hbm, wk_hbm, wv_hbm, wo_hbm, out_hbm,
            xs, a_loc, w, wo, k_s, vt_s, q_s, top_s, mix_s, s_s, peak_s, y_own, from_mate, from_far, half_in,
            w_send, w_recv, w_fwd, x_loc, x_mate_send, x_mate, x_send, x_dir, x_fwd_send, x_fwd,
            mate_send, mate_recv, half_send, half_recv, far_send, far_recv, misc):
    me = lax.axis_index("sp")
    y = lax.axis_index("dp")
    xx, cc = lax.div(me, 2), lax.rem(me, 2)
    mate = 2 * xx + 1 - cc
    far = 2 * (1 - xx) + cc
    far0 = 2 * (1 - xx)
    weights = (wk_hbm, wv_hbm, wq_hbm)
    rows = B // 2
    depth = 256

    barrier = pltpu.get_barrier_semaphore()
    for peer in (mate, far, 2 * (1 - xx) + 1 - cc):
        pl.semaphore_signal(barrier, inc=1, device_id={"dp": y, "sp": peer}, device_id_type=MESH)
    pl.semaphore_signal(barrier, inc=1, device_id={"dp": 1 - y, "sp": me}, device_id_type=MESH)
    pl.semaphore_wait(barrier, 4)

    def remote(src, dst, send, recv, sp, dp=y):
        return pltpu.make_async_remote_copy(src_ref=src, dst_ref=dst, send_sem=send, recv_sem=recv, device_id={"dp": dp, "sp": sp},
                                            device_id_type=MESH)

    def w_place(m, hp, sender):
        return w.at[m, hp, pl.ds(pl.multiple_of(sender * depth, depth), depth), :]

    def w_columns(m, hp, owner):
        return weights[m].at[:, pl.ds(pl.multiple_of(owner * 1024 + hp * 256, 256), 256)]

    def w_to(m, hp, owner, n):
        return remote(w_columns(m, hp, owner), w_place(m, hp, me), w_send.at[m, hp, n], w_recv.at[m, hp, me], owner)

    def w_from(m, hp, sender):
        return remote(w_place(m, hp, sender), w_place(m, hp, sender), misc.at[0], w_recv.at[m, hp, sender], sender)

    def w_on(m, hp, n):
        place = w_place(m, hp, far0 + n)
        return remote(place, place, w_fwd.at[m, lax.div(hp, 2), n], w_recv.at[m, hp, far0 + n], me, 1 - y)

    def w_own(m, hp):
        return pltpu.make_async_copy(w_columns(m, hp, me), w_place(m, hp, me), w_recv.at[m, hp, me])

    def x_own(i):
        return pltpu.make_async_copy(x_hbm.at[pl.ds(i * B, B), :], xs.at[2 * me + i], x_loc.at[i])

    def x_to_mate(i):
        return remote(x_hbm.at[pl.ds(i * B, B), :], xs.at[2 * me + i], x_mate_send.at[i], x_mate.at[i], mate)

    def x_from_mate(i):
        return remote(xs.at[2 * mate + i], xs.at[2 * mate + i], misc.at[0], x_mate.at[i], mate)

    def x_half(b, c):
        return xs.at[b, pl.ds(pl.multiple_of(c * rows, rows), rows), :]

    def x_to_far(i):
        return remote(x_half(4 * xx + i, cc), x_half(4 * xx + i, cc), x_send.at[i], x_dir.at[i], far)

    def x_from_far(i):
        place = x_half(4 * (1 - xx) + i, cc)
        return remote(place, place, misc.at[0], x_dir.at[i], far)

    def x_on(i):
        place = x_half(4 * (1 - xx) + i, cc)
        return remote(place, place, x_fwd_send.at[i], x_fwd.at[i], mate)

    def x_on_from(i):
        place = x_half(4 * (1 - xx) + i, 1 - cc)
        return remote(place, place, misc.at[0], x_fwd.at[i], mate)

    def y_to_mate(i, h):
        cols, k = pl.ds(h * 512, 512), lax.rem(i, 2)
        return remote(a_loc.at[i, :, cols], from_mate.at[k, :, cols], mate_send.at[k, h], mate_recv.at[k, h], mate)

    def y_from_mate(i, h):
        place = from_mate.at[i, :, pl.ds(h * 512, 512)]
        return remote(place, place, misc.at[0], mate_recv.at[i, h], mate)

    def half_to_mate(i):
        return remote(x_half(4 * (1 - xx) + i, 1 - cc), half_in.at[i], half_send.at[i], half_recv.at[i], mate)

    def half_from_mate(i):
        return remote(half_in.at[i], half_in.at[i], misc.at[0], half_recv.at[i], mate)

    def y_to_far(i):
        owner = 2 * (1 - xx) + lax.div(i, 2)
        return remote(x_half(4 * (1 - xx) + i, cc), from_far.at[lax.rem(i, 2), cc], far_send.at[i], far_recv.at[lax.rem(i, 2), cc], owner)

    def y_from_far(i, c):
        return remote(from_far.at[i, c], from_far.at[i, c], misc.at[0], far_recv.at[i, c], far0 + c)

    def loop(n, body):
        lax.fori_loop(0, n, lambda i, _: (body(i), None)[1], None)

    def hp_at(it):
        return 2 * lax.div(it, 2) + jnp.where(lax.rem(it, 2) == 0, y, 1 - y)

    def crossing(g):
        if isinstance(g, int) and g < 6:
            return [w_to(g % 3, hp_at(2 * (g // 3)), far0 + (cc if n == 1 else 1 - cc), n) for n in (1, 2)]
        return [x_to_far(g - 6)]

    def cross(g):
        for copy in crossing(g - 2):
            copy.wait_send()
        for copy in crossing(g):
            copy.start()

    for g in range(2):
        for copy in crossing(g):
            copy.start()
    for i in range(2):
        x_own(i).start()
        x_to_mate(i).start()
    for it in range(4):
        hp = hp_at(it)
        for m in range(3):
            w_own(m, hp).start()
            w_to(m, hp, mate, 0).start()
    wo_copy = pltpu.make_async_copy(wo_hbm, wo, misc.at[1])
    wo_copy.start()

    def arrive(m, hp, onward):
        for n in range(2):
            w_from(m, hp, far0 + n).wait_recv()
            if onward:
                w_on(m, hp, n).start()

    arrive(0, hp_at(0), True)
    cross(2)
    for i in range(2):
        x_own(i).wait()
    for i in range(2):
        x_from_mate(i).wait_recv()

    gain = gain_ref[...].astype(jnp.float32)[None, :]

    def norm_rows(src, dst, here):
        wide = src[here, :].astype(jnp.float32)
        scale = lax.rsqrt(jnp.mean(wide * wide, -1, keepdims=True) + 1e-6)
        dst[here, :] = (wide * scale * gain).astype(jnp.bfloat16)

    def norm(src, dst):
        loop(B // 256, lambda r: norm_rows(src, dst, pl.ds(pl.multiple_of(r * 256, 256), 256)))

    def turn_table(b):
        cos, sin = [], []
        for r in range(B // 64):
            at = pl.ds(b * (B // 64) + r, 1)
            ch, sh, cf, sf = ang_ref[0, at, :], ang_ref[1, at, :], ang_ref[2], ang_ref[3]
            cos.append(ch * cf - sh * sf)
            sin.append(sh * cf + ch * sf)
        return jnp.concatenate(cos, axis=0), jnp.concatenate(sin, axis=0)

    def turned(t, table):
        t = t.astype(jnp.float32)
        return (t * table[0] + pltpu.roll(t, 64, 1) * table[1]).astype(jnp.bfloat16)

    def project(a, m, hp, b, slot, table):
        t = _dot(a[...], w[m, hp], 1, 0).astype(jnp.bfloat16)
        for i in range(2):
            part = t[:, i * HEAD : (i + 1) * HEAD]
            if m == 0:
                k_s[b, 2 * hp + i] = turned(part, table)
            elif m == 1:
                vt_s[b, 2 * hp + i] = part.T
            else:
                q_s[slot, 2 * hp + i] = turned(part, table)

    e = HEAD**-0.5 * LOG2E

    half = B // 2
    halves = [(n, slice(at, at + half)) for n in range(QUAD) for at in (0, half)]

    def scores(j, slot, quad, n, cols):
        s = _dot(k_s[j, quad * QUAD + n], q_s[slot, quad * QUAD + n, cols, :], 1, 1)
        peak_s[n : n + 1, cols] = s.max(axis=0, keepdims=True)
        s_s[n, :, cols] = s

    def values(j, h, keys):
        return jnp.concatenate([vt_s[j, h, :, 0:keys], jnp.ones((16, keys), jnp.bfloat16)], axis=0)

    def attend(qb, slot, quad, lo, hi, after, *, diagonal=True, state=0, first=True, final=True, between=None, sizes=(2, 1)):
        @pl.when(first)
        def _():
            for n, cols in halves:
                scores(lo, slot, quad, n, cols)

        def whole(j):
            more = diagonal | (j + 1 < hi)
            key, where, which = jnp.where(more, j + 1, after[0]), jnp.where(more, slot, after[1]), jnp.where(more, quad, after[2])
            for n, cols in halves:
                old = top_s[state, n : n + 1, cols]
                top = jnp.maximum(old, peak_s[n : n + 1, cols])
                top_s[state, n : n + 1, cols] = top
                p = jnp.exp2((s_s[n, :, cols] - top) * e).astype(jnp.bfloat16)
                scores(key, where, which, n, cols)
                mix_s[state, n, :, cols] = mix_s[state, n, :, cols] * jnp.exp2((old - top) * e) + _dot(values(j, quad * QUAD + n, B), p, 1, 0)

        def finish():
            for n in range(QUAD):
                out = mix_s[state, n, 0:HEAD, :] * (1 / mix_s[state, n, HEAD : HEAD + 1, :])
                q_s[slot, quad * QUAD + n] = out.T.astype(jnp.bfloat16)
                mix_s[state, n] = jnp.zeros(mix_s.shape[2:], jnp.float32)
            top_s[state] = jnp.full(top_s.shape[1:], NEG, jnp.float32)

        count, at = hi - lo, lo
        for size in sizes:
            turns = lax.div(count, size)
            turn = lambda t, size=size, at=at: [whole(at + size * t + n) for n in range(size)] and None
            if size == sizes[0] and len(sizes) > 1:
                loop(turns, turn)
            else:
                pl.when(turns == 1)(functools.partial(turn, 0))
            at, count = at + size * turns, count - size * turns

        if between is not None:
            between()

        @pl.when(diagonal)
        def _():
            ok = lax.broadcasted_iota(jnp.int32, (half, half), 1) >= lax.broadcasted_iota(jnp.int32, (half, half), 0)
            for n in range(QUAD):
                h = quad * QUAD + n
                for at in (0, half):
                    cols = slice(at, at + half)
                    parts = [s_s[n, 0:half, cols], jnp.where(ok, s_s[n, half:B, cols], HIDDEN)] if at else [jnp.where(ok, s_s[n, 0:half, cols], HIDDEN)]
                    old = top_s[state, n : n + 1, cols]
                    top = old
                    for part in parts:
                        top = jnp.maximum(top, part.max(axis=0, keepdims=True))
                    top_s[state, n : n + 1, cols] = top
                    p = jnp.concatenate([jnp.exp2((part - top) * e).astype(jnp.bfloat16) for part in parts], axis=0)
                    mix_s[state, n, :, cols] = mix_s[state, n, :, cols] * jnp.exp2((old - top) * e) + _dot(values(qb, h, at + half), p, 1, 0)
                    if at:
                        for c in (slice(0, half), slice(half, B)):
                            scores(after[0], after[1], after[2], n, c)
            if final is True:
                finish()

        if final is not True:
            pl.when(final)(finish)
        elif diagonal is not True:
            pl.when(jnp.logical_not(diagonal))(finish)

    def combine(i):
        def part(r):
            here = pl.ds(pl.multiple_of(cc * rows + r * 64, 64), 64)
            at = pl.ds(pl.multiple_of(r * 64, 64), 64)
            b = 4 * (1 - xx) + i
            xs[b, here, :] = (xs[b, here, :].astype(jnp.float32) + half_in[i, at, :].astype(jnp.float32)).astype(jnp.bfloat16)

        loop(rows // 64, part)

    top_s[...] = jnp.full(top_s.shape, NEG, jnp.float32)
    mix_s[...] = jnp.zeros(mix_s.shape, jnp.float32)
    loop(4, lambda i: norm(xs.at[4 * xx + i], a_loc.at[i]))

    def pair(it):
        hp = hp_at(it)

        def when(n, work):
            @pl.when(it == n)
            def _():
                for m, at, onward, then in work:
                    arrive(m, hp_at(at), onward)
                    if then is not None:
                        cross(then)

        for m in range(3):
            w_own(m, hp).wait()
            w_from(m, hp, mate).wait_recv()
            when(0, [[], [(1, 0, True, 3)], [(2, 0, True, 4)]][m])
            when(1, [[(0, 1, False, None)], [(1, 1, False, None)], [(0, 2, True, 5), (2, 1, False, None)]][m])
            when(2, [[], [], [(2, 2, True, 7)]][m])
            when(3, [(m, 3, False, None)])
            for i in range(4):
                b = 4 * xx + i
                project(a_loc.at[i], m, hp, b, i, None if m == 1 else turn_table(b))

        @pl.when((it == 1) | (it == 2) | ((it == 3) & (xx == 1)))
        def _():
            blk = jnp.where(it == 2, 2, 3)
            short = it == 3
            quad = jnp.where(short, 1, 0)
            attend(4 * xx + blk, blk, quad, 4 * xx, 4 * xx + blk - quad, (jnp.where(short, 6, 0), 3, quad), diagonal=jnp.logical_not(short),
                   state=xx * jnp.where(it == 1, 1, jnp.where(short, 2, 3)), final=xx == 0, between=lambda: when(1, [(1, 2, True, 6)]))

    loop(4, pair)
    wo_copy.wait()

    first = 1 - xx

    def forward_x(i):
        x_from_far(i).wait_recv()
        x_on(i).start()

    def x_here(i):
        x_on(i).wait_send()
        x_on_from(i).wait_recv()

    a_far = a_loc.at[2 * cc]

    @pl.when(xx == 1)
    def _():
        forward_x(0)
        attend(7, 3, 1, 6, 7, (0, 4, 0), state=2, first=False, final=False, sizes=(1,))

    def blocks(s):
        i = s - first
        away = (i >= 0) & (i < 4)
        qb = jnp.where(xx == 1, s, jnp.where(s < 1, s, jnp.where(s < 5, s + 3, s - 4)))
        here = qb - 4 * xx
        return i, away, qb, here, jnp.where(away, 4, here)

    def step(s):
        @pl.when((s == 1) | (s == 2))
        def _():
            cross(s + 7)

        i, away, qb, here, slot = blocks(s)
        next_slot = blocks(s + 1)[-1]

        @pl.when(i == 0)
        def _():
            x_here(0)
            norm(xs.at[qb], a_far)

        @pl.when(away)
        def _():
            table = turn_table(qb)
            for hp in range(4):
                for m in range(3):
                    project(a_far, m, hp, qb, 4, table)
                if hp == 1:
                    for n, cols in halves:
                        scores(0, 4, 0, n, cols)

        def quad(n):
            resume = (xx == 1) & ((s == 7) | ((s == 6) & (n == 0)))

            @pl.when(jnp.logical_not((xx == 0) & (s >= 6) & (n == 0)))
            def _():
                attend(qb, slot, n, 0, jnp.where(resume, 4, qb),
                       (0, jnp.where(n == 0, slot, next_slot), jnp.where((n == 0) | ((s >= 5) & (xx == 0)), 1, 0)),
                       diagonal=jnp.logical_not(resume), state=jnp.where(resume, jnp.where(s == 7, 1 + n, 3), 0),
                       first=(n == 0) & (s == 0), sizes=(4, 2, 1))

            @pl.when((n == 0) & (i >= -1) & (i < 3))
            def _():
                forward_x(i + 1)

            @pl.when((n == 0) & (i >= 1) & (i < 5))
            def _():
                half_from_mate(i - 1).wait_recv()
                combine(i - 1)
                y_to_far(i - 1).start()

        loop(8 // QUAD, quad)

        own = jnp.logical_not(away) & (lax.div(here, 2) == cc)

        def output(store):
            seen = jnp.concatenate([q_s[slot, h] for h in range(8)], axis=1)
            for n in range(4):
                cols = slice(n * 256, n * 256 + 256)
                store(cols, _dot(seen, wo[:, cols], 1, 0))

        @pl.when(own)
        def _():
            def store(cols, r):
                y_own[lax.rem(here, 2), :, cols] = r

            output(store)

        @pl.when(away & (i < 3))
        def _():
            x_here(i + 1)

        @pl.when(away)
        def _():
            after = 4 * (1 - xx) + jnp.minimum(i + 1, 3)
            for r in range(B // 64):
                norm_rows(xs.at[after], a_far, slice(r * 64, r * 64 + 64))

            def store(cols, r):
                xs[qb, :, cols] = r.astype(jnp.bfloat16)

            output(store)

        @pl.when(jnp.logical_not(own | away))
        def _():
            def store(cols, r):
                a_loc[here, :, cols] = r.astype(jnp.bfloat16)
                if cols.stop % 512 == 0:
                    y_to_mate(here, cols.stop // 512 - 1).start()

            output(store)

        @pl.when(away)
        def _():
            half_to_mate(i).start()

    loop(8, step)

    for i in range(2):
        for h in range(2):
            y_from_mate(i, h).wait_recv()
        for c in range(2):
            y_from_far(i, c).wait_recv()
            base = c * rows

            def part(r):
                here = pl.ds(pl.multiple_of(base + r * 128, 128), 128)
                at = pl.ds(pl.multiple_of(r * 128, 128), 128)
                f = jnp.float32
                total = y_own[i, here, :] + from_mate[i, here, :].astype(f) + from_far[i, c, at, :].astype(f)
                a_loc[2 * cc + i, here, :] = (xs[2 * me + i, here, :].astype(f) + total).astype(jnp.bfloat16)

            loop(rows // 128, part)
        pltpu.make_async_copy(a_loc.at[2 * cc + i], out_hbm.at[pl.ds(i * B, B), :], x_loc.at[i]).start()

    for i in range(2):
        x_to_mate(i).wait_send()
        for h in range(2):
            y_to_mate(2 * (1 - cc) + i, h).wait_send()
    for it in range(4):
        hp = hp_at(it)
        for m in range(3):
            w_to(m, hp, mate, 0).wait_send()
            if it % 2 == 0:
                for n in range(2):
                    w_on(m, hp, n).wait_send()

    for i in (2, 3):
        x_to_far(i).wait_send()

    def last(i):
        half_to_mate(i).wait_send()
        y_to_far(i).wait_send()

    loop(4, last)
    for i in range(2):
        pltpu.make_async_copy(a_loc.at[2 * cc + i], out_hbm.at[pl.ds(i * B, B), :], x_loc.at[i]).wait()


def solution(mesh):
    bf, f = jnp.bfloat16, jnp.float32
    dma = pltpu.SemaphoreType.DMA

    def step(x, gain, wq, wk, wv, wo):
        hbm = pl.BlockSpec(memory_space=pl.ANY)
        vmem = pl.BlockSpec(memory_space=pltpu.VMEM)
        return pl.pallas_call(
            _kernel,
            out_shape=jax.ShapeDtypeStruct(x.shape, bf),
            in_specs=[hbm, vmem, vmem, hbm, hbm, hbm, hbm],
            out_specs=hbm,
            scratch_shapes=[
                pltpu.VMEM((8, B, 1024), bf),
                pltpu.VMEM((4, B, 1024), bf),
                pltpu.VMEM((3, 4, 1024, 256), bf),
                pltpu.VMEM((1024, 1024), bf),
                pltpu.VMEM((8, 8, B, HEAD), bf),
                pltpu.VMEM((8, 8, HEAD, B), bf),
                pltpu.VMEM((5, 8, B, HEAD), bf),
                pltpu.VMEM((4, QUAD, B), f),
                pltpu.VMEM((4, QUAD, HEAD + 16, B), f),
                pltpu.VMEM((QUAD, B, B), f),
                pltpu.VMEM((QUAD, B), f),
                pltpu.VMEM((2, B, 1024), f),
                pltpu.VMEM((2, B, 1024), bf),
                pltpu.VMEM((2, 2, B // 2, 1024), bf),
                pltpu.VMEM((4, B // 2, 1024), bf),
                dma((3, 4, 3)), dma((3, 4, 4)), dma((3, 2, 2)),
                dma((2,)), dma((2,)), dma((2,)), dma((4,)), dma((4,)), dma((4,)), dma((4,)),
                dma((2, 2)), dma((2, 2)), dma((4,)), dma((4,)), dma((4,)), dma((2, 2)), dma((2,)),
            ],
            compiler_params=pltpu.CompilerParams(collective_id=0, has_side_effects=True, vmem_limit_bytes=67043328),
            name="layer",
        )(x, gain, _angles(), wq, wk, wv, wo)

    tokens, whole = P(("dp", "sp"), None), P("sp", None)
    return jax.shard_map(
        step,
        mesh=mesh,
        in_specs=(tokens, P(None), whole, whole, whole, whole),
        out_specs=tokens,
        check_vma=False,
    )
```
